256 devices in a mesh: region: 16 (over z, x_hi), feat: 4 (over x_lo, core), row: 4 (over y).
Axes of the slice: x: 4 (x_hi: 2, x_lo: 2; x = x_hi * 2 + x_lo), y: 4, z: 8, core: 2. Of those that a mesh axis runs over, the one named last changes fastest.
Arguments:
- samples: bfloat16 [524288, 128], P(('region', 'row')), may hold values from -6 to 6
- targets: bfloat16 [524288, 64], P(('region', 'row')), may hold values from -6 to 6
- member: int32 [524288], P(('region', 'row')), may hold values 0 or 1
- omega: bfloat16 [128, 4096], P(None, 'feat'), may hold values from -0.5 to 0.5
- phase: float32 [4096], P('feat'), may hold values from -3.140625 to 3.140625
- factors: float32 [65536, 1024], P(('region', 'feat')), may hold values from -0.08 to 5, as said below
- weights_init: float32 [65536, 64], P(('region', 'feat'), 'row'), may hold values from -3 to 3
- duals_init: float32 [65536, 64], P(('region', 'feat'), 'row'), may hold values from -2 to 2
- consensus_init: float32 [4096, 64], P('feat', 'row'), may hold values from -3 to 3
- penalty_init: float32 [16], P('region'), may hold values from 2 to 8
Outputs:
- weights: float32 [65536, 64], P(('region', 'feat'), 'row')
- duals: float32 [65536, 64], P(('region', 'feat'), 'row')
- consensus: float32 [4096, 64], P('feat', 'row')
- penalty: float32 [16, 3], P('region')
The draws below stay inside these ranges and needn't reach their ends.
Inputs may be any that keep to these rules, and one draw needn't show every extreme that they name: factors: each 1024 x 1024 block is lower triangular, its diagonal between 3.5 and 5, its entries below the diagonal drawn independently, symmetric about zero and at most 0.08 in magnitude.
All inputs are finite; a program needn't handle non-finite values. No bound on the sum of `member` on one device may be relied on, other than what follows from the above.
Results may differ from the reference program's by a relative error of at most 0.006.
Values may be sent and summed in bfloat16 or wider, within the bound.
A program may use at most 128 MiB of HBM per device.

```python
import math
import jax
import jax.numpy as jnp
from jax import lax

INPUTS = 128
FEATURES = 4096
OUTPUTS = 64
ITERS = 3
BLOCK = 1024
REGIONS = 16
SAMPLES = 32768
N_FEAT = 4


def draw_samples(key, part):
    first_key, second_key = jax.random.split(jax.random.fold_in(key, 17))
    shape = (REGIONS * SAMPLES, INPUTS)
    values = jax.random.uniform(first_key, shape, jnp.float32, -6.0, 6.0)
    return values.astype(jnp.bfloat16)


def draw_factors(key, part):
    first_key, second_key = jax.random.split(key)
    height = REGIONS * FEATURES
    below = jnp.clip(jax.random.normal(first_key, (height, BLOCK), jnp.float32), -4.0, 4.0) * 0.02
    diagonal = jax.random.uniform(second_key, (height, 1), jnp.float32, 3.5, 5.0)
    inside = jnp.arange(height) % BLOCK
    column = jnp.arange(BLOCK)
    lower = jnp.where(column[None, :] < inside[:, None], below, 0.0)
    return lower + jnp.where(column[None, :] == inside[:, None], diagonal, 0.0)


def set_ends(result, stream_key, least, top_value):
    longest = result.shape.index(max(result.shape))
    spots = []
    for shift in (0, 1):
        where = [jax.random.randint(jax.random.fold_in(stream_key, axis), (), 0, length) for axis, length in enumerate(result.shape)]
        where[longest] = (where[longest] + shift) % result.shape[longest]
        spots.append(tuple(where))
    return result.at[spots[0]].set(least).at[spots[1]].set(top_value)


def shard_levels(stream_key, extent, pieces, low, high):
    level, own = 1.0, jax.random.fold_in(stream_key, 6)
    for dim, shards_of in pieces:
        steps = jnp.exp(jax.random.uniform(jax.random.fold_in(own, dim), (shards_of,), jnp.float32, low / len(pieces), high / len(pieces)))
        level = level * jnp.repeat(steps, extent[dim] // shards_of).reshape([-1 if axis == dim else 1 for axis in range(len(extent))])
    return level


def gaussian(key, extent, spread, limit, pieces=(), held_as=jnp.bfloat16):
    result = jax.random.normal(key, extent, jnp.float32) * spread
    if len(pieces) > 0:
        result = shard_levels(key, extent, pieces, -0.22, 0.18) * result
    return jnp.clip(result, min=-limit, max=limit).astype(held_as)


def setup_inputs(seed: int = 0) -> dict:
    key_list = jax.random.split(jax.random.key(seed), 11)
    samples = draw_samples(jax.random.fold_in(key_list[10], 71), 0)
    targets = gaussian(key_list[1], (REGIONS * SAMPLES, OUTPUTS), 1.0, 6.0, ((0, 64),))
    member = set_ends((jax.random.randint(key_list[2], (REGIONS * SAMPLES,), 0, 8) < 7).astype(jnp.int32), jax.random.fold_in(key_list[2], 1), 0, 1)
    omega = gaussian(key_list[3], (INPUTS, FEATURES), INPUTS ** -0.5, 0.5, ((1, 4),))
    phase = jnp.clip(jax.random.uniform(key_list[4], (FEATURES,), jnp.float32, -3.140625, 3.140625), -3.140625, 3.140625)
    factors = draw_factors(jax.random.fold_in(key_list[10], 71), 0)
    weights_init = gaussian(key_list[6], (REGIONS * FEATURES, OUTPUTS), 0.5, 3.0, ((0, 64), (1, 4)), jnp.float32)
    duals_init = gaussian(key_list[7], (REGIONS * FEATURES, OUTPUTS), 0.3, 2.0, ((0, 64), (1, 4)), jnp.float32)
    consensus_init = gaussian(key_list[8], (FEATURES, OUTPUTS), 0.5, 3.0, ((0, 4), (1, 4)), jnp.float32)
    penalty_init = jnp.clip(jnp.exp(math.log(8.0) - 1.3862944 * jax.random.uniform(key_list[9], (REGIONS,), jnp.float32) ** shard_levels(key_list[9], (REGIONS,), ((0, 16),), -0.2, 0.2)), 2.0, 8.0)
    return {"samples": samples, "targets": targets, "member": member, "omega": omega, "phase": phase, "factors": factors, "weights_init": weights_init, "duals_init": duals_init, "consensus_init": consensus_init, "penalty_init": penalty_init}


def features_of(inputs, omega, phase):
    angle = jnp.dot(inputs.astype(jnp.float32), omega.astype(jnp.float32), preferred_element_type=jnp.float32) + phase
    return (math.sqrt(2.0 / FEATURES) * jnp.cos(angle)).astype(jnp.bfloat16)

def block_solve(factor, right_side):
    forward = lax.linalg.triangular_solve(factor, right_side, left_side=True, lower=True)
    return lax.linalg.triangular_solve(factor, forward, left_side=True, lower=True, transpose_a=True)

def reference(samples, targets, member, omega, phase, factors, weights_init, duals_init, consensus_init, penalty_init):
    inputs = samples.reshape(REGIONS, SAMPLES, INPUTS)
    wanted = targets.reshape(REGIONS, SAMPLES, OUTPUTS)
    chosen = member.reshape(REGIONS, SAMPLES)
    blocks = factors.reshape(REGIONS, N_FEAT, BLOCK, BLOCK)
    weights = weights_init.reshape(REGIONS, FEATURES, OUTPUTS)
    duals = duals_init.reshape(REGIONS, FEATURES, OUTPUTS)
    consensus = consensus_init
    penalty = penalty_init
    offset = 0.01 * FEATURES * OUTPUTS
    history = []
    for iteration in range(ITERS):

        def region_step(items):
            region_in, region_out, region_mask, region_factor, local, dual, scalar = items
            features = features_of(region_in, omega, phase)
            predicted = jnp.dot(features.astype(jnp.float32), local.astype(jnp.bfloat16).astype(jnp.float32), preferred_element_type=jnp.float32)
            residual = (region_mask.astype(jnp.float32)[:, None] * (predicted - region_out.astype(jnp.float32))).astype(jnp.bfloat16)
            gradient = lax.dot_general(features.astype(jnp.float32), residual.astype(jnp.float32), (((0,), (0,)), ((), ())), preferred_element_type=jnp.float32)
            right_side = gradient + scalar * (local - consensus + dual)
            update = jax.vmap(block_solve)(region_factor, right_side.reshape(N_FEAT, BLOCK, OUTPUTS))
            return local - update.reshape(FEATURES, OUTPUTS)
        weights = lax.map(region_step, (inputs, wanted, chosen, blocks, weights, duals, penalty))
        scaled = penalty[:, None, None]
        updated = lax.optimization_barrier(jnp.sum(scaled * (weights + duals), axis=0)) / jnp.sum(penalty)
        duals = duals + weights - updated
        gap = lax.optimization_barrier(jnp.sum(jnp.square(weights - updated), axis=(1, 2)))
        drift = penalty * penalty * jnp.sum(jnp.square(updated - consensus))
        renewed = penalty * jnp.sqrt((gap + offset) / (drift + offset))
        duals = duals * (penalty / renewed)[:, None, None]
        consensus = updated
        penalty = renewed
        history.append(renewed)
    return (weights.reshape(REGIONS * FEATURES, OUTPUTS), duals.reshape(REGIONS * FEATURES, OUTPUTS), consensus, jnp.stack(history, axis=1))
```

```python
import math

import jax
import jax.numpy as jnp
from jax import lax
from jax.experimental import pallas as pl
from jax.experimental.pallas import tpu as pltpu
from jax.sharding import PartitionSpec as P

FEATURES = 4096
OUTPUTS = 64
ITERS = 3
REGIONS = 16
ROWS = 4
FEATS = 4
BLOCK = 1024
INPUTS = 128
CHIP = 4096
HALF = 2048
SLICE = 16
MESH = pl.DeviceIdType.MESH
F32 = jnp.float32
BF16 = jnp.bfloat16
SINE = (6.2831640442521435, -41.33714236464144, 81.34076868066526, -70.99343137755689)
NT = (((1,), (1,)), ((), ()))


def dot(a, b):
    return jnp.dot(a, b, preferred_element_type=F32)


def dot_nt(a, b):
    return lax.dot_general(a, b, NT, preferred_element_type=F32)


def remote(src, dst, send, recv, device):
    return pltpu.make_async_remote_copy(
        src_ref=src,
        dst_ref=dst,
        send_sem=send,
        recv_sem=recv,
        device_id=device,
        device_id_type=MESH,
    )


def kernel(
    samples,
    targets,
    member,
    omega,
    phase,
    factors,
    w_in,
    u_in,
    z_in,
    rho_in,
    w_out,
    u_out,
    z_out,
    pen_out,
    feat,
    twice,
    omegas,
    phases,
    rhs,
    tgt,
    mem,
    low,
    inv,
    weights,
    own,
    pred_send,
    pred_recv,
    res_own,
    res_other,
    acc,
    grad_send,
    grad_recv,
    cons_src,
    cons_sum,
    cons_all,
    gaps,
    w,
    u,
    z,
    local,
    om_s,
    om_r,
    ag_s,
    ag_r,
    rs_s,
    rs_r,
    pair_s,
    pair_r,
    cs_s,
    cs_r,
    ca_s,
    ca_r,
    gp_s,
    gp_r,
):
    reg = lax.axis_index("region")
    f = lax.axis_index("feat")
    y = lax.axis_index("row")
    core = lax.rem(f, 2)
    xl = f // 2
    xh = lax.rem(reg, 2)
    partner = (reg, xl * 2 + 1 - core, y)

    def chip(k):
        dx, dy = divmod(k, ROWS)
        return lax.rem(xl + dx, 2), lax.rem(y + dy, ROWS)

    def chip_device(k):
        tx, ty = chip(k)
        return (reg, tx * 2 + core, ty)

    def group_device(k):
        df, dy = divmod(k, ROWS)
        return (reg, lax.rem(f + df, FEATS), lax.rem(y + dy, ROWS))

    def region_device(k):
        return (lax.rem(reg + k, REGIONS), f, y)

    across = (reg, (1 - xl) * 2 + core, y)
    beside = (reg - xh + 1 - xh, (1 - xl) * 2 + core, y)

    mine = pl.ds(pl.multiple_of(xl * CHIP, CHIP), CHIP)
    half = xl * CHIP + core * HALF
    loads = [
        pltpu.make_async_copy(omega, omegas.at[xl], local.at[0]),
        pltpu.make_async_copy(phase, phases.at[xl], local.at[1]),
        pltpu.make_async_copy(samples.at[mine, :], twice.at[:, pl.ds(0, INPUTS)], local.at[2]),
        pltpu.make_async_copy(
            samples.at[mine, :], twice.at[:, pl.ds(INPUTS, INPUTS)], local.at[3]
        ),
        pltpu.make_async_copy(
            targets.at[:, pl.ds(pl.multiple_of(half, HALF), HALF)], tgt, local.at[4]
        ),
        pltpu.make_async_copy(
            member.at[pl.ds(pl.multiple_of(half // 128, 16), 16), :], mem, local.at[5]
        ),
        pltpu.make_async_copy(factors, low, local.at[6]),
    ]
    for load in loads:
        load.start()

    barrier = pltpu.get_barrier_semaphore()
    for k in range(1, FEATS * ROWS):
        pl.semaphore_signal(barrier, inc=1, device_id=group_device(k), device_id_type=MESH)
    for k in range(1, REGIONS):
        pl.semaphore_signal(barrier, inc=1, device_id=region_device(k), device_id_type=MESH)
    pl.semaphore_signal(barrier, inc=1, device_id=beside, device_id_type=MESH)

    w[...] = w_in[...]
    u[...] = u_in[...]
    z[...] = z_in[...]
    weights[0, xl, y] = w_in[...].astype(BF16)

    for load in loads[:4]:
        load.wait()

    scale = math.sqrt(2.0 / FEATURES)
    c1, c3, c5, c7 = (-scale * c for c in SINE)

    def make_features(j):
        turns = omegas[j].astype(F32) * (0.5 / math.pi)
        high = turns.astype(BF16)
        rhs[pl.ds(0, INPUTS), :] = high
        rhs[pl.ds(INPUTS, INPUTS), :] = (turns - high.astype(F32)).astype(BF16)
        shift = phases[j] * (0.5 / math.pi)

        def body(i, _):
            for m in range(2):
                rows = pl.ds(pl.multiple_of(i * 512 + m * 256, 256), 256)
                lhs = twice[rows, :]
                for n in range(4):
                    cols = pl.ds(n * 256, 256)
                    turn = dot(lhs, rhs[:, cols]) + shift[:, n * 256 : n * 256 + 256]
                    g = jnp.abs(turn - jnp.round(turn)) - 0.25
                    s = g * g
                    feat[j, rows, cols] = (g * (c1 + s * (c3 + s * (c5 + s * c7)))).astype(BF16)
            return 0

        lax.fori_loop(0, CHIP // 512, body, 0)

    make_features(xl)

    pl.semaphore_wait(barrier, 31)

    om = [
        remote(
            omegas.at[xl, pl.ds(0, 64), :],
            omegas.at[xl, pl.ds(0, 64), :],
            om_s.at[0],
            om_r.at[0],
            across,
        ),
        remote(
            omegas.at[xl, pl.ds(64, 64), :],
            omegas.at[xl, pl.ds(64, 64), :],
            om_s.at[1],
            om_r.at[1],
            beside,
        ),
        remote(phases.at[xl], phases.at[xl], om_s.at[2], om_r.at[2], across),
    ]
    om_in = [
        remote(
            omegas.at[1 - xl, pl.ds(0, 64), :],
            omegas.at[1 - xl, pl.ds(0, 64), :],
            om_s.at[0],
            om_r.at[0],
            across,
        ),
        remote(
            omegas.at[1 - xl, pl.ds(64, 64), :],
            omegas.at[1 - xl, pl.ds(64, 64), :],
            om_s.at[1],
            om_r.at[1],
            beside,
        ),
        remote(phases.at[1 - xl], phases.at[1 - xl], om_s.at[2], om_r.at[2], across),
    ]
    for copy in om:
        copy.start()

    def gather(it):
        return [
            remote(
                weights.at[it, xl, y],
                weights.at[it, xl, y],
                ag_s.at[it, k],
                ag_r.at[it, k],
                chip_device(k),
            )
            for k in range(1, 8)
        ]

    def gather_in(it):
        out = []
        for k in range(1, 8):
            dx, dy = divmod(k, ROWS)
            sx, sy = lax.rem(xl + dx, 2), lax.rem(y + ROWS - dy, ROWS)
            out.append(
                remote(
                    weights.at[it, sx, sy],
                    weights.at[it, sx, sy],
                    ag_s.at[it, k],
                    ag_r.at[it, k],
                    chip_device(k),
                )
            )
        return out

    sent = list(om)

    def start(copies):
        for copy in copies:
            copy.start()
        sent.extend(copies)

    start_gather = gather(0)
    start(start_gather)

    for copy in om_in:
        copy.wait_recv()
    make_features(1 - xl)

    eye = lax.broadcasted_iota(jnp.int32, (128, 128), 0) == lax.broadcasted_iota(
        jnp.int32, (128, 128), 1
    )

    def make_inverse():
        ys, qs, columns, lanes = [], [], [], []
        inv[...] = jnp.zeros_like(inv)
        for b in range(8):
            at = pl.ds(b * 128, 128)
            block = low[at, at]
            diagonal = jnp.where(eye, block, 0.0)
            column = 1.0 / jnp.sum(diagonal, axis=1, keepdims=True)
            lanes.append(1.0 / jnp.sum(diagonal, axis=0, keepdims=True))
            columns.append(column)
            n = jnp.where(eye, 0.0, block) * column
            ys.append(-n)
            qs.append(dot(n.astype(BF16), n.astype(BF16)))
        for step in range(6):
            for b in range(8):
                q = qs[b].astype(BF16)
                if step < 5:
                    both = dot(jnp.concatenate([ys[b].astype(BF16), q], axis=0), q)
                    ys[b] = ys[b] + qs[b] + both[:128]
                    qs[b] = both[128:]
                else:
                    ys[b] = ys[b] + qs[b] + dot(ys[b].astype(BF16), q)
        for b in range(8):
            at = pl.ds(b * 128, 128)
            inv[at, at] = ys[b].astype(BF16)
        size = 128
        while size < BLOCK:
            for top in range(0, BLOCK, 2 * size):
                a = pl.ds(top, size)
                b = pl.ds(top + size, size)
                column = jnp.concatenate(
                    columns[(top + size) // 128 : (top + 2 * size) // 128], axis=0
                )
                c = low[b, a] * column
                t = c + dot(inv[b, b], c.astype(BF16))
                t = t + dot(t.astype(BF16), inv[a, a])
                inv[b, a] = (-t).astype(BF16)
            size *= 2
        return jnp.concatenate(lanes, axis=1)

    def predict(it, first):
        def body(i, _):
            for m in range(2):
                at = pl.multiple_of(i * 512 + m * 256, 256)
                rows = pl.ds(pl.multiple_of(first + at, 256), 256)
                both = dot_nt(weights[it, 0].reshape(OUTPUTS, BLOCK), feat[0, rows, :])
                both += dot_nt(weights[it, 1].reshape(OUTPUTS, BLOCK), feat[1, rows, :])
                own[:, pl.ds(at, 256)] = both
            return 0

        lax.fori_loop(0, HALF // 512, body, 0)

    def scale_to(value, shape):
        return jnp.broadcast_to(value, shape)

    def consensus_send(it, rho):
        value = scale_to(rho, (SLICE, BLOCK)) * (w[...] + u[...])
        for k in range(REGIONS):
            r, c = divmod(k, 8)
            cons_src[it, k, 0] = value[r * 8 : r * 8 + 8, c * 128 : c * 128 + 128]
            cons_src[it, k, 1] = scale_to(rho, (8, 128))
        cons_sum[it, reg] = cons_src[it, reg]
        start(
            [
                remote(
                    cons_src.at[it, lax.rem(reg + k, REGIONS)],
                    cons_sum.at[it, reg],
                    cs_s.at[it, k],
                    cs_r.at[it, k],
                    region_device(k),
                )
                for k in range(1, REGIONS)
            ]
        )

    def consensus_sum(it):
        for k in range(1, REGIONS):
            came = lax.rem(reg + REGIONS - k, REGIONS)
            remote(
                cons_src.at[it, came],
                cons_sum.at[it, came],
                cs_s.at[it, k],
                cs_r.at[it, k],
                region_device(k),
            ).wait_recv()
        total = cons_sum[it, 0]
        for k in range(1, REGIONS):
            total = total + cons_sum[it, k]
        cons_all[it, reg] = total[0] / total[1]
        start(
            [
                remote(
                    cons_all.at[it, reg],
                    cons_all.at[it, reg],
                    ca_s.at[it, k],
                    ca_r.at[it, k],
                    region_device(k),
                )
                for k in range(1, REGIONS)
            ]
        )

    def consensus_take(it):
        for k in range(1, REGIONS):
            came = lax.rem(reg + REGIONS - k, REGIONS)
            remote(
                cons_all.at[it, came],
                cons_all.at[it, came],
                ca_s.at[it, k],
                ca_r.at[it, k],
                region_device(k),
            ).wait_recv()
        gap = jnp.zeros((8, 128), F32)
        drift = jnp.zeros((8, 128), F32)
        for k in range(REGIONS):
            r, c = divmod(k, 8)
            at = (pl.ds(r * 8, 8), pl.ds(c * 128, 128))
            new = cons_all[it, k]
            apart = w[at] - new
            moved = new - z[at]
            gap += apart * apart
            drift += moved * moved
            u[at] = u[at] + apart
            z[at] = new
        row = lax.broadcasted_iota(jnp.int32, (8, 128), 0)
        gap = scale_to(jnp.sum(gap, axis=0, keepdims=True), (8, 128))
        drift = scale_to(jnp.sum(drift, axis=0, keepdims=True), (8, 128))
        me = f * ROWS + y
        gaps[it, me] = jnp.where(row == 0, gap, jnp.where(row == 1, drift, 0.0))
        start(
            [
                remote(
                    gaps.at[it, me], gaps.at[it, me], gp_s.at[it, k], gp_r.at[it, k], group_device(k)
                )
                for k in range(1, FEATS * ROWS)
            ]
        )

    def penalty(it, rho):
        for k in range(1, FEATS * ROWS):
            df, dy = divmod(k, ROWS)
            came = lax.rem(f + FEATS - df, FEATS) * ROWS + lax.rem(y + ROWS - dy, ROWS)
            remote(
                gaps.at[it, came], gaps.at[it, came], gp_s.at[it, k], gp_r.at[it, k], group_device(k)
            ).wait_recv()
        total = gaps[it, 0]
        for k in range(1, FEATS * ROWS):
            total = total + gaps[it, k]
        total = jnp.sum(total, axis=1, keepdims=True)
        offset = 0.01 * FEATURES * OUTPUTS
        gap, drift = total[0:1], rho * rho * total[1:2]
        new = rho * jnp.sqrt((gap + offset) / (drift + offset))
        u[...] = u[...] * scale_to(rho / new, (SLICE, BLOCK))
        pen_out[:, it : it + 1] = new
        return new

    for load in loads[4:]:
        load.wait()

    rho = jnp.full((1, 1), rho_in[0], F32)
    lanes = None
    mine_at = pl.multiple_of(core * HALF, HALF)
    other_at = pl.multiple_of((1 - core) * HALF, HALF)
    for it in range(ITERS):
        for copy in gather_in(it):
            copy.wait_recv()
        predict(it, other_at)
        pred_send[it] = own[...].astype(BF16)
        pred = remote(pred_send.at[it], pred_recv.at[it], pair_s.at[it, 0], pair_r.at[it, 0], partner)
        start([pred])
        predict(it, mine_at)
        if it:
            consensus_sum(it - 1)
        pred.wait_recv()
        for g in range(HALF // 128):
            at = pl.ds(g * 128, 128)
            value = own[:, at] + pred_recv[it, :, at].astype(F32) - tgt[:, at].astype(F32)
            res_own[it, :, at] = (mem[g : g + 1, :].astype(F32) * value).astype(BF16)
        res = remote(res_own.at[it], res_other.at[it], pair_s.at[it, 1], pair_r.at[it, 1], partner)
        start([res])

        def first_half(j, _):
            for n in range(4):
                cols = pl.ds(n * 256, 256)
                acc[j, :, cols] = dot(res_own[it], feat[j, pl.ds(mine_at, HALF), cols])
            return 0

        lax.fori_loop(0, 2, first_half, 0)
        res.wait_recv()
        for side in (1, 0):
            j = lax.rem(xl + side, 2)

            def second_half(n, _):
                cols = pl.ds(pl.multiple_of(n * 256, 256), 256)
                total = acc[j, :, cols] + dot(res_other[it], feat[j, pl.ds(other_at, HALF), cols])
                grad_send[it, j, :, :, cols] = total.reshape(ROWS, SLICE, 256).astype(BF16)
                return 0

            for n in range(4):
                second_half(n, 0)
            start(
                [
                    remote(
                        grad_send.at[it, chip(k)[0], chip(k)[1]],
                        grad_recv.at[it, k],
                        rs_s.at[it, k],
                        rs_r.at[it, k],
                        chip_device(k),
                    )
                    for k in range(side * 4, side * 4 + 4)
                    if k
                ]
            )
        if it == 0:
            lanes = make_inverse()
        else:
            consensus_take(it - 1)
            rho = penalty(it - 1, rho)
        gradient = grad_send[it, xl, y].astype(F32)
        for k in range(1, 8):
            remote(
                grad_send.at[it, 0, 0], grad_recv.at[it, k], rs_s.at[it, k], rs_r.at[it, k], across
            ).wait_recv()
        for k in range(1, 8):
            gradient = gradient + grad_recv[it, k].astype(F32)
        right = gradient + scale_to(rho, (SLICE, BLOCK)) * (w[...] - z[...] + u[...])
        right = right * lanes
        right = right + dot_nt(right.astype(BF16), inv[...])
        right = right + dot(right.astype(BF16), inv[...])
        new = w[...] - right * lanes
        w[...] = new
        if it < ITERS - 1:
            weights[it + 1, xl, y] = new.astype(BF16)
            start(gather(it + 1))
        consensus_send(it, rho)

    w_out[...] = w[...]
    consensus_sum(ITERS - 1)
    consensus_take(ITERS - 1)
    penalty(ITERS - 1, rho)
    u_out[...] = u[...]
    z_out[...] = z[...]
    for copy in sent:
        copy.wait_send()


def per_device(
    samples,
    targets,
    member,
    omega,
    phase,
    factors,
    weights_init,
    duals_init,
    consensus_init,
    penalty_init,
):
    hbm = pl.BlockSpec(memory_space=pl.ANY)
    vmem = pl.BlockSpec(memory_space=pltpu.VMEM)
    smem = pl.BlockSpec(memory_space=pltpu.SMEM)
    state = jax.ShapeDtypeStruct((SLICE, BLOCK), F32)
    dma = pltpu.SemaphoreType.DMA
    w, u, z, pen = pl.pallas_call(
        kernel,
        out_shape=(state, state, state, jax.ShapeDtypeStruct((1, ITERS), F32)),
        in_specs=[hbm] * 6 + [vmem] * 3 + [smem],
        out_specs=(vmem,) * 4,
        scratch_shapes=[
            pltpu.VMEM((2, CHIP, BLOCK), BF16),
            pltpu.VMEM((CHIP, 2 * INPUTS), BF16),
            pltpu.VMEM((2, INPUTS, BLOCK), BF16),
            pltpu.VMEM((2, 1, BLOCK), F32),
            pltpu.VMEM((2 * INPUTS, BLOCK), BF16),
            pltpu.VMEM((OUTPUTS, HALF), BF16),
            pltpu.VMEM((16, 128), jnp.int32),
            pltpu.VMEM((BLOCK, BLOCK), F32),
            pltpu.VMEM((BLOCK, BLOCK), BF16),
            pltpu.VMEM((ITERS, 2, ROWS, SLICE, BLOCK), BF16),
            pltpu.VMEM((OUTPUTS, HALF), F32),
            pltpu.VMEM((ITERS, OUTPUTS, HALF), BF16),
            pltpu.VMEM((ITERS, OUTPUTS, HALF), BF16),
            pltpu.VMEM((ITERS, OUTPUTS, HALF), BF16),
            pltpu.VMEM((ITERS, OUTPUTS, HALF), BF16),
            pltpu.VMEM((2, OUTPUTS, BLOCK), F32),
            pltpu.VMEM((ITERS, 2, ROWS, SLICE, BLOCK), BF16),
            pltpu.VMEM((ITERS, 8, SLICE, BLOCK), BF16),
            pltpu.VMEM((ITERS, REGIONS, 2, 8, 128), F32),
            pltpu.VMEM((ITERS, REGIONS, 2, 8, 128), F32),
            pltpu.VMEM((ITERS, REGIONS, 8, 128), F32),
            pltpu.VMEM((ITERS, FEATS * ROWS, 8, 128), F32),
            pltpu.VMEM((SLICE, BLOCK), F32),
            pltpu.VMEM((SLICE, BLOCK), F32),
            pltpu.VMEM((SLICE, BLOCK), F32),
            dma((7,)),
            dma((3,)),
            dma((3,)),
            dma((ITERS, 8)),
            dma((ITERS, 8)),
            dma((ITERS, 8)),
            dma((ITERS, 8)),
            dma((ITERS, 2)),
            dma((ITERS, 2)),
            dma((ITERS, REGIONS)),
            dma((ITERS, REGIONS)),
            dma((ITERS, REGIONS)),
            dma((ITERS, REGIONS)),
            dma((ITERS, REGIONS)),
            dma((ITERS, REGIONS)),
        ],
        compiler_params=pltpu.CompilerParams(
            collective_id=0, has_side_effects=True, vmem_limit_bytes=60 * 1024 * 1024
        ),
        name="admm",
    )(
        samples,
        targets.T,
        member.reshape(64, 128),
        omega,
        phase.reshape(1, BLOCK),
        factors,
        weights_init.T,
        duals_init.T,
        consensus_init.T,
        penalty_init,
    )
    return w.T, u.T, z.T, pen


def solution(mesh):
    return jax.shard_map(
        per_device,
        mesh=mesh,
        in_specs=(
            P(("region", "row"), None),
            P(("region", "row"), None),
            P(("region", "row")),
            P(None, "feat"),
            P("feat"),
            P(("region", "feat"), None),
            P(("region", "feat"), "row"),
            P(("region", "feat"), "row"),
            P("feat", "row"),
            P("region"),
        ),
        out_specs=(
            P(("region", "feat"), "row"),
            P(("region", "feat"), "row"),
            P("feat", "row"),
            P("region", None),
        ),
        check_vma=False,
    )
```

```python
import math

import jax
import jax.numpy as jnp
from jax import lax
from jax.experimental import pallas as pl
from jax.experimental.pallas import tpu as pltpu
from jax.sharding import PartitionSpec as P

FEATURES = 4096
OUTPUTS = 64
ITERS = 3
REGIONS = 16
ROWS = 4
FEATS = 4
BLOCK = 1024
INPUTS = 128
CHIP = 4096
HALF = 2048
SLICE = 16
MESH = pl.DeviceIdType.MESH
F32 = jnp.float32
BF16 = jnp.bfloat16
SINE = (6.2831640442521435, -41.33714236464144, 81.34076868066526, -70.99343137755689)
NT = (((1,), (1,)), ((), ()))
scope = jax.named_scope


def dot(a, b):
    return jnp.dot(a, b, preferred_element_type=F32)


def dot_nt(a, b):
    return lax.dot_general(a, b, NT, preferred_element_type=F32)


def remote(src, dst, send, recv, device):
    return pltpu.make_async_remote_copy(
        src_ref=src,
        dst_ref=dst,
        send_sem=send,
        recv_sem=recv,
        device_id=device,
        device_id_type=MESH,
    )


def kernel(
    samples,
    targets,
    member,
    omega,
    phase,
    factors,
    w_in,
    u_in,
    z_in,
    rho_in,
    w,
    u,
    z,
    pen_out,
    feat_mine,
    feat_other,
    sample,
    omegas,
    phases,
    rhs,
    turns_next,
    tgt,
    mem,
    low,
    inv,
    weights,
    pred,
    pred_send,
    pred_recv,
    res_own,
    res_other,
    acc,
    grad_send,
    grad_recv,
    cons_src,
    cons_sum,
    cons_all,
    rhos,
    gaps,
    local,
    om_s,
    om_r,
    ag_s,
    ag_r,
    rs_s,
    rs_r,
    pair_s,
    pair_r,
    cs_s,
    cs_r,
    ca_s,
    ca_r,
    gp_s,
    gp_r,
    ro_s,
    ro_r,
):
    reg = lax.axis_index("region")
    f = lax.axis_index("feat")
    y = lax.axis_index("row")
    core = lax.rem(f, 2)
    xl = f // 2
    xh = lax.rem(reg, 2)
    partner = (reg, xl * 2 + 1 - core, y)

    def chip(k):
        dx, dy = divmod(k, ROWS)
        return lax.rem(xl + dx, 2), lax.rem(y + dy, ROWS)

    def chip_device(k):
        tx, ty = chip(k)
        return (reg, tx * 2 + core, ty)

    def group_device(k):
        df, dy = divmod(k, ROWS)
        return (reg, lax.rem(f + df, FEATS), lax.rem(y + dy, ROWS))

    def region_device(k):
        return (lax.rem(reg + k, REGIONS), f, y)

    across = (reg, (1 - xl) * 2 + core, y)
    beside = (reg - xh + 1 - xh, (1 - xl) * 2 + core, y)

    first = xl * CHIP
    half = xl * CHIP + core * HALF
    early = 1024

    def rows_of(start, size):
        return pl.ds(pl.multiple_of(start, 128), size)

    loads = [
        pltpu.make_async_copy(omega, omegas.at[0], local.at[0]),
        pltpu.make_async_copy(phase, phases.at[0], local.at[1]),
        pltpu.make_async_copy(
            samples.at[rows_of(first, early), :], sample.at[pl.ds(0, early), :], local.at[2]
        ),
        pltpu.make_async_copy(w_in, w, local.at[3]),
        pltpu.make_async_copy(
            samples.at[rows_of(first + early, CHIP - early), :],
            sample.at[pl.ds(early, CHIP - early), :],
            local.at[4],
        ),
        pltpu.make_async_copy(u_in, u, local.at[5]),
        pltpu.make_async_copy(z_in, z, local.at[6]),
        pltpu.make_async_copy(targets.at[:, rows_of(half, HALF)], tgt, local.at[7]),
        pltpu.make_async_copy(
            member.at[pl.ds(pl.multiple_of(half // 128, 16), 16), :], mem, local.at[8]
        ),
        pltpu.make_async_copy(factors, low, local.at[9]),
    ]
    for load in loads:
        load.start()

    barrier = pltpu.get_barrier_semaphore()
    for k in range(1, FEATS * ROWS):
        pl.semaphore_signal(barrier, inc=1, device_id=group_device(k), device_id_type=MESH)
    for k in range(1, REGIONS):
        pl.semaphore_signal(barrier, inc=1, device_id=region_device(k), device_id_type=MESH)
    pl.semaphore_signal(barrier, inc=1, device_id=beside, device_id_type=MESH)

    with scope("load"):
        for load in loads[:3]:
            load.wait()

    scale = math.sqrt(2.0 / FEATURES)
    c1, c3, c5, c7 = (-scale * c for c in SINE)

    def make_rhs(side):
        turns = omegas[side].astype(F32) * (0.5 / math.pi)
        high = turns.astype(BF16)
        rest = (turns - high.astype(F32)).astype(BF16)
        for n in range(8):
            rhs[n, pl.ds(0, INPUTS), :] = high[:, n * 128 : n * 128 + 128]
            rhs[n, pl.ds(INPUTS, INPUTS), :] = rest[:, n * 128 : n * 128 + 128]

    def turns_of(row, n):
        block = sample[rows_of(row, 256), :]
        return dot(
            jnp.concatenate([block, block], axis=1),
            jnp.concatenate([rhs[2 * n], rhs[2 * n + 1]], axis=1),
        )

    def weights_of(it, side):
        return weights[it, side].reshape(OUTPUTS, BLOCK)

    def make_features(side, base, count, predicting):
        feat = feat_other if side else feat_mine
        shift = phases[side] * (0.5 / math.pi)
        turns_next[...] = turns_of(base, 0)

        def body(i, _):
            tiles = [(m, n) for m in range(2) for n in range(4)]
            now = turns_next[...]
            total = None
            for t, (m, n) in enumerate(tiles):
                row = base + i * 512 + m * 256
                if t + 1 < len(tiles):
                    later = turns_of(base + i * 512 + tiles[t + 1][0] * 256, tiles[t + 1][1])
                else:
                    later = turns_of(base + jnp.minimum(i + 1, count - 1) * 512, 0)
                turn = now + shift[:, n * 256 : n * 256 + 256]
                g = jnp.abs(turn - jnp.round(turn)) - 0.25
                s = g * g
                value = (g * (c1 + s * (c3 + s * (c5 + s * c7)))).astype(BF16)
                rows = rows_of(row, 256)
                feat[2 * n, rows, :] = value[:, :128]
                feat[2 * n + 1, rows, :] = value[:, 128:]
                if predicting:
                    cols = slice(n * 256, n * 256 + 256)
                    before = jnp.concatenate(
                        [feat_mine[2 * n, rows, :], feat_mine[2 * n + 1, rows, :]], axis=1
                    )
                    part = dot_nt(weights_of(0, 0)[:, cols], before)
                    part += dot_nt(weights_of(0, 1)[:, cols], value)
                    total = part if n == 0 else total + part
                    if n == 3:
                        pred[:, rows] = total
                now = later
            turns_next[...] = now
            return 0

        lax.fori_loop(0, count, body, 0)

    with scope("features_mine"):
        make_rhs(0)
        make_features(0, 0, 2, False)

    with scope("barrier"):
        pl.semaphore_wait(barrier, 31)

    om = [
        remote(
            omegas.at[0, pl.ds(0, 64), :],
            omegas.at[1, pl.ds(0, 64), :],
            om_s.at[0],
            om_r.at[0],
            across,
        ),
        remote(
            omegas.at[0, pl.ds(64, 64), :],
            omegas.at[1, pl.ds(64, 64), :],
            om_s.at[1],
            om_r.at[1],
            beside,
        ),
        remote(phases.at[0], phases.at[1], om_s.at[2], om_r.at[2], across),
    ]
    sent = []

    def start(copies):
        for copy in copies:
            copy.start()
        sent.extend(copies)

    start(om)

    def gather(it):
        return [
            remote(
                weights.at[it, 0, y],
                weights.at[it, k // ROWS, y],
                ag_s.at[it, k],
                ag_r.at[it, k],
                chip_device(k),
            )
            for k in range(1, 8)
        ]

    def gather_wait(it, ks):
        for k in ks:
            dx, dy = divmod(k, ROWS)
            came = lax.rem(y + ROWS - dy, ROWS)
            remote(
                weights.at[it, 0, y],
                weights.at[it, dx, came],
                ag_s.at[it, k],
                ag_r.at[it, k],
                chip_device(k),
            ).wait_recv()

    def send_rho(it, rho):
        rhos[it, reg] = jnp.broadcast_to(rho, (1, 128))
        start(
            [
                remote(
                    rhos.at[it, reg], rhos.at[it, reg], ro_s.at[it, k], ro_r.at[it, k], region_device(k)
                )
                for k in range(1, REGIONS)
            ]
        )

    loads[3].wait()
    weights[0, 0, y] = w[...].astype(BF16)
    start(gather(0))
    rho = jnp.full((1, 1), rho_in[0], F32)
    send_rho(0, rho)

    loads[4].wait()
    with scope("features_mine_rest"):
        make_features(0, early, (CHIP - early) // 512, False)

    with scope("omega_wait"):
        for copy in om:
            copy.wait_recv()

    eye = lax.broadcasted_iota(jnp.int32, (128, 128), 0) == lax.broadcasted_iota(
        jnp.int32, (128, 128), 1
    )

    def make_inverse():
        ys, qs, columns, lanes = [], [], [], []
        inv[...] = jnp.zeros_like(inv)
        for b in range(8):
            at = pl.ds(b * 128, 128)
            block = low[at, at]
            diagonal = jnp.where(eye, block, 0.0)
            column = 1.0 / jnp.sum(diagonal, axis=1, keepdims=True)
            lanes.append(1.0 / jnp.sum(diagonal, axis=0, keepdims=True))
            columns.append(column)
            n = jnp.where(eye, 0.0, block) * column
            ys.append(-n)
            qs.append(dot(n.astype(BF16), n.astype(BF16)))
        for step in range(6):
            for b in range(8):
                q = qs[b].astype(BF16)
                if step < 5:
                    both = dot(jnp.concatenate([ys[b].astype(BF16), q], axis=0), q)
                    ys[b] = ys[b] + qs[b] + both[:128]
                    qs[b] = both[128:]
                else:
                    ys[b] = ys[b] + qs[b] + dot(ys[b].astype(BF16), q)
        for b in range(8):
            inv[b, pl.ds(b * 128, 128), :] = ys[b].astype(BF16)

        def square(top, size):
            return jnp.concatenate(
                [inv[top // 128 + i, pl.ds(top, size), :] for i in range(size // 128)], axis=1
            )

        size = 128
        while size < BLOCK:
            for top in range(0, BLOCK, 2 * size):
                column = jnp.concatenate(
                    columns[(top + size) // 128 : (top + 2 * size) // 128], axis=0
                )
                c = low[pl.ds(top + size, size), pl.ds(top, size)] * column
                t = c + dot(square(top + size, size), c.astype(BF16))
                t = (-t - dot(t.astype(BF16), square(top, size))).astype(BF16)
                for i in range(size // 128):
                    inv[top // 128 + i, pl.ds(top + size, size), :] = t[:, i * 128 : i * 128 + 128]
            size *= 2
        return jnp.concatenate(lanes, axis=1)

    def predict(it, side, base, count, more):
        feat = feat_other if side else feat_mine

        def body(i, _):
            for m in range(4):
                rows = rows_of(base + i * 1024 + m * 256, 256)
                block = jnp.concatenate([feat[n, rows, :] for n in range(8)], axis=1)
                part = dot_nt(weights_of(it, side), block)
                pred[:, rows] = pred[:, rows] + part if more else part
            return 0

        lax.fori_loop(0, count, body, 0)

    def scale_to(value, shape):
        return jnp.broadcast_to(value, shape)

    def consensus_send(it, rho):
        value = scale_to(rho, (SLICE, BLOCK)) * (w[...] + u[...])
        for k in range(REGIONS):
            r, c = divmod(k, 8)
            cons_src[it, k] = value[r * 8 : r * 8 + 8, c * 128 : c * 128 + 128]
        cons_sum[it, reg] = cons_src[it, reg]
        start(
            [
                remote(
                    cons_src.at[it, lax.rem(reg + k, REGIONS)],
                    cons_sum.at[it, reg],
                    cs_s.at[it, k],
                    cs_r.at[it, k],
                    region_device(k),
                )
                for k in range(1, REGIONS)
            ]
        )

    def consensus_sum(it):
        with scope("sum_wait"):
            for k in range(1, REGIONS):
                came = lax.rem(reg + REGIONS - k, REGIONS)
                remote(
                    cons_src.at[it, came],
                    cons_sum.at[it, came],
                    cs_s.at[it, k],
                    cs_r.at[it, k],
                    region_device(k),
                ).wait_recv()
                remote(
                    rhos.at[it, came], rhos.at[it, came], ro_s.at[it, k], ro_r.at[it, k], region_device(k)
                ).wait_recv()
        total, divisor = cons_sum[it, 0], rhos[it, 0]
        for k in range(1, REGIONS):
            total = total + cons_sum[it, k]
            divisor = divisor + rhos[it, k]
        cons_all[it, reg] = total / divisor
        start(
            [
                remote(
                    cons_all.at[it, reg],
                    cons_all.at[it, reg],
                    ca_s.at[it, k],
                    ca_r.at[it, k],
                    region_device(k),
                )
                for k in range(1, REGIONS)
            ]
        )

    def consensus_take(it):
        with scope("take_wait"):
            for k in range(1, REGIONS):
                came = lax.rem(reg + REGIONS - k, REGIONS)
                remote(
                    cons_all.at[it, came],
                    cons_all.at[it, came],
                    ca_s.at[it, k],
                    ca_r.at[it, k],
                    region_device(k),
                ).wait_recv()
        gap = jnp.zeros((8, 128), F32)
        drift = jnp.zeros((8, 128), F32)
        for k in range(REGIONS):
            r, c = divmod(k, 8)
            at = (pl.ds(r * 8, 8), pl.ds(c * 128, 128))
            new = cons_all[it, k]
            apart = w[at] - new
            moved = new - z[at]
            gap += apart * apart
            drift += moved * moved
            u[at] = u[at] + apart
            z[at] = new
        row = lax.broadcasted_iota(jnp.int32, (2, 128), 0)
        gap = scale_to(jnp.sum(gap, axis=0, keepdims=True), (2, 128))
        drift = scale_to(jnp.sum(drift, axis=0, keepdims=True), (2, 128))
        me = f * ROWS + y
        gaps[it, me] = jnp.where(row == 0, gap, drift)
        start(
            [
                remote(
                    gaps.at[it, me], gaps.at[it, me], gp_s.at[it, k], gp_r.at[it, k], group_device(k)
                )
                for k in range(1, FEATS * ROWS)
            ]
        )

    def penalty(it, rho):
        with scope("gap_wait"):
            for k in range(1, FEATS * ROWS):
                df, dy = divmod(k, ROWS)
                came = lax.rem(f + FEATS - df, FEATS) * ROWS + lax.rem(y + ROWS - dy, ROWS)
                remote(
                    gaps.at[it, came],
                    gaps.at[it, came],
                    gp_s.at[it, k],
                    gp_r.at[it, k],
                    group_device(k),
                ).wait_recv()
        total = gaps[it, 0]
        for k in range(1, FEATS * ROWS):
            total = total + gaps[it, k]
        total = jnp.sum(total, axis=1, keepdims=True)
        offset = 0.01 * FEATURES * OUTPUTS
        gap, drift = total[0:1], rho * rho * total[1:2]
        new = rho * jnp.sqrt((gap + offset) / (drift + offset))
        u[...] = u[...] * scale_to(rho / new, (SLICE, BLOCK))
        pen_out[:, it : it + 1] = new
        return new

    mine_at = core * HALF
    other_at = (1 - core) * HALF
    lanes = None
    for it in range(ITERS):
        if it == 0:
            with scope("gather_wait"):
                gather_wait(0, range(1, 8))
            with scope("features_other"):
                make_rhs(1)
                make_features(1, other_at, 4, True)
        else:
            with scope("gather_wait"):
                gather_wait(it, range(1, 4))
            with scope("predict_first"):
                predict(it, 0, 0, 4, False)
            with scope("gather_wait"):
                gather_wait(it, range(4, 8))
            with scope("predict_other"):
                predict(it, 1, other_at, 2, True)
        for g in range(HALF // 128):
            pred_send[it, g] = pred[:, rows_of(other_at + g * 128, 128)].astype(BF16)
        to_pair = remote(
            pred_send.at[it], pred_recv.at[it], pair_s.at[it, 0], pair_r.at[it, 0], partner
        )
        start([to_pair])
        if it == 0:
            with scope("features_other_rest"):
                make_features(1, mine_at, 4, True)
            for load in loads[5:]:
                load.wait()
        else:
            consensus_sum(it - 1)
            with scope("predict_mine"):
                predict(it, 1, mine_at, 2, True)
        with scope("pred_wait"):
            to_pair.wait_recv()
        with scope("residual"):
            for g in range(HALF // 128):
                value = pred[:, rows_of(mine_at + g * 128, 128)] + pred_recv[it, g].astype(F32)
                value = value - tgt[:, g * 128 : g * 128 + 128].astype(F32)
                res_own[it, g] = (mem[g : g + 1, :].astype(F32) * value).astype(BF16)
        res = remote(res_own.at[it], res_other.at[it], pair_s.at[it, 1], pair_r.at[it, 1], partner)
        start([res])

        def gradient_part(residual, feat, at, n):
            rows = rows_of(at, HALF)
            return dot(
                jnp.concatenate([residual[it, g] for g in range(HALF // 128)], axis=1),
                jnp.concatenate([feat[2 * n, rows, :], feat[2 * n + 1, rows, :]], axis=1),
            )

        with scope("gradient_mine"):
            for side, feat in ((1, feat_other), (0, feat_mine)):
                for n in range(4):
                    acc[side, :, pl.ds(n * 256, 256)] = gradient_part(res_own, feat, mine_at, n)
        if it:
            consensus_take(it - 1)
        with scope("res_wait"):
            res.wait_recv()
        for side, feat in ((1, feat_other), (0, feat_mine)):
            with scope("gradient_other"):
                for n in range(4):
                    cols = pl.ds(n * 256, 256)
                    total = acc[side, :, cols] + gradient_part(res_other, feat, other_at, n)
                    grad_send[it, side, :, :, cols] = total.reshape(ROWS, SLICE, 256).astype(BF16)
            start(
                [
                    remote(
                        grad_send.at[it, side, chip(k)[1]],
                        grad_recv.at[it, k],
                        rs_s.at[it, k],
                        rs_r.at[it, k],
                        chip_device(k),
                    )
                    for k in range(side * 4, side * 4 + 4)
                    if k
                ]
            )
        if it == 0:
            with scope("inverse"):
                lanes = make_inverse()
        else:
            rho = penalty(it - 1, rho)
            send_rho(it, rho)
        gradient = grad_send[it, 0, y].astype(F32)
        with scope("grad_wait"):
            for k in range(1, 8):
                remote(
                    grad_send.at[it, 0, 0],
                    grad_recv.at[it, k],
                    rs_s.at[it, k],
                    rs_r.at[it, k],
                    chip_device(k),
                ).wait_recv()
        with scope("solve"):
            for k in range(1, 8):
                gradient = gradient + grad_recv[it, k].astype(F32)
            right = gradient + scale_to(rho, (SLICE, BLOCK)) * (w[...] - z[...] + u[...])
            right = right * lanes
            inverse = jnp.concatenate([inv[n] for n in range(8)], axis=1)
            right = right + dot_nt(right.astype(BF16), inverse)
            right = right + dot(right.astype(BF16), inverse)
            new = w[...] - right * lanes
            w[...] = new
        if it < ITERS - 1:
            weights[it + 1, 0, y] = new.astype(BF16)
            start(gather(it + 1))
        with scope("consensus_send"):
            consensus_send(it, rho)

    consensus_sum(ITERS - 1)
    consensus_take(ITERS - 1)
    penalty(ITERS - 1, rho)
    for copy in sent:
        copy.wait_send()


def hand_over(*refs):
    for source, out in zip(refs[:4], refs[4:]):
        out[...] = source[...]


def per_device(
    samples,
    targets,
    member,
    omega,
    phase,
    factors,
    weights_init,
    duals_init,
    consensus_init,
    penalty_init,
):
    hbm = pl.BlockSpec(memory_space=pl.ANY)
    vmem = pl.BlockSpec(memory_space=pltpu.VMEM)
    smem = pl.BlockSpec(memory_space=pltpu.SMEM)
    state = jax.ShapeDtypeStruct((SLICE, BLOCK), F32)
    dma = pltpu.SemaphoreType.DMA
    w, u, z, pen = pl.pallas_call(
        kernel,
        out_shape=(state, state, state, jax.ShapeDtypeStruct((1, ITERS), F32)),
        in_specs=[hbm] * 9 + [smem],
        out_specs=(vmem,) * 4,
        scratch_shapes=[
            pltpu.VMEM((8, CHIP, 128), BF16),
            pltpu.VMEM((8, CHIP, 128), BF16),
            pltpu.VMEM((CHIP, INPUTS), BF16),
            pltpu.VMEM((2, INPUTS, BLOCK), BF16),
            pltpu.VMEM((2, 1, BLOCK), F32),
            pltpu.VMEM((8, 2 * INPUTS, 128), BF16),
            pltpu.VMEM((256, 256), F32),
            pltpu.VMEM((OUTPUTS, HALF), BF16),
            pltpu.VMEM((16, 128), jnp.int32),
            pltpu.VMEM((BLOCK, BLOCK), F32),
            pltpu.VMEM((8, BLOCK, 128), BF16),
            pltpu.VMEM((ITERS, 2, ROWS, SLICE, BLOCK), BF16),
            pltpu.VMEM((OUTPUTS, CHIP), F32),
            pltpu.VMEM((ITERS, 16, OUTPUTS, 128), BF16),
            pltpu.VMEM((ITERS, 16, OUTPUTS, 128), BF16),
            pltpu.VMEM((ITERS, 16, OUTPUTS, 128), BF16),
            pltpu.VMEM((ITERS, 16, OUTPUTS, 128), BF16),
            pltpu.VMEM((2, OUTPUTS, BLOCK), F32),
            pltpu.VMEM((ITERS, 2, ROWS, SLICE, BLOCK), BF16),
            pltpu.VMEM((ITERS, 8, SLICE, BLOCK), BF16),
            pltpu.VMEM((ITERS, REGIONS, 8, 128), F32),
            pltpu.VMEM((ITERS, REGIONS, 8, 128), F32),
            pltpu.VMEM((ITERS, REGIONS, 8, 128), F32),
            pltpu.VMEM((ITERS, REGIONS, 1, 128), F32),
            pltpu.VMEM((ITERS, FEATS * ROWS, 2, 128), F32),
            dma((10,)),
            dma((3,)),
            dma((3,)),
            dma((ITERS, 8)),
            dma((ITERS, 8)),
            dma((ITERS, 8)),
            dma((ITERS, 8)),
            dma((ITERS, 2)),
            dma((ITERS, 2)),
            dma((ITERS, REGIONS)),
            dma((ITERS, REGIONS)),
            dma((ITERS, REGIONS)),
            dma((ITERS, REGIONS)),
            dma((ITERS, REGIONS)),
            dma((ITERS, REGIONS)),
            dma((ITERS, REGIONS)),
            dma((ITERS, REGIONS)),
        ],
        compiler_params=pltpu.CompilerParams(
            collective_id=0, has_side_effects=True, vmem_limit_bytes=60 * 1024 * 1024
        ),
        name="admm",
    )(
        samples,
        targets.T,
        member.reshape(64, 128),
        omega,
        phase.reshape(1, BLOCK),
        factors,
        weights_init.T,
        duals_init.T,
        consensus_init.T,
        penalty_init,
    )
    w, u, z, pen = pl.pallas_call(
        hand_over,
        out_shape=(state, state, state, jax.ShapeDtypeStruct((1, ITERS), F32)),
        in_specs=[vmem] * 4,
        out_specs=(vmem,) * 4,
        name="hand_over",
    )(w, u, z, pen)
    return w.T, u.T, z.T, pen


def solution(mesh):
    return jax.shard_map(
        per_device,
        mesh=mesh,
        in_specs=(
            P(("region", "row"), None),
            P(("region", "row"), None),
            P(("region", "row")),
            P(None, "feat"),
            P("feat"),
            P(("region", "feat"), None),
            P(("region", "feat"), "row"),
            P(("region", "feat"), "row"),
            P("feat", "row"),
            P("region"),
        ),
        out_specs=(
            P(("region", "feat"), "row"),
            P(("region", "feat"), "row"),
            P("feat", "row"),
            P("region", None),
        ),
        check_vma=False,
    )
```

```python
import math

import jax
import jax.numpy as jnp
from jax import lax
from jax.experimental import pallas as pl
from jax.experimental.pallas import tpu as pltpu
from jax.sharding import PartitionSpec as P

FEATURES = 4096
OUTPUTS = 64
ITERS = 3
REGIONS = 16
ROWS = 4
FEATS = 4
BLOCK = 1024
INPUTS = 128
CHIP = 4096
HALF = 2048
SLICE = 16
MESH = pl.DeviceIdType.MESH
F32 = jnp.float32
BF16 = jnp.bfloat16
SINE = (6.2831640442521435, -41.33714236464144, 81.34076868066526, -70.99343137755689)
PIECES = 4
NT = (((1,), (1,)), ((), ()))
scope = jax.named_scope


def dot(a, b):
    return jnp.dot(a, b, preferred_element_type=F32)


def dot_nt(a, b):
    return lax.dot_general(a, b, NT, preferred_element_type=F32)


def remote(src, dst, send, recv, device):
    return pltpu.make_async_remote_copy(
        src_ref=src,
        dst_ref=dst,
        send_sem=send,
        recv_sem=recv,
        device_id=device,
        device_id_type=MESH,
    )


def kernel(
    samples,
    targets,
    member,
    omega,
    phase,
    factors,
    w_in,
    u_in,
    z_in,
    rho_in,
    w,
    u,
    z,
    pen_out,
    feat_mine,
    feat_other,
    turned_mine,
    turned_other,
    sample,
    omegas,
    phases,
    rhs,
    turns_next,
    tgt,
    mem,
    low,
    inv,
    inv_t,
    weights,
    pred,
    pred_send,
    pred_recv,
    res_own,
    res_other,
    acc,
    grad_send,
    grad_recv,
    cons_src,
    cons_sum,
    cons_all,
    rhos,
    gaps,
    local,
    om_s,
    om_r,
    ag_s,
    ag_r,
    rs_s,
    rs_r,
    pair_s,
    pair_r,
    cs_s,
    cs_r,
    ca_s,
    ca_r,
    gp_s,
    gp_r,
    ro_s,
    ro_r,
):
    reg = lax.axis_index("region")
    f = lax.axis_index("feat")
    y = lax.axis_index("row")
    core = lax.rem(f, 2)
    xl = f // 2
    xh = lax.rem(reg, 2)
    partner = (reg, xl * 2 + 1 - core, y)

    def chip(k):
        dx, dy = divmod(k, ROWS)
        return lax.rem(xl + dx, 2), lax.rem(y + dy, ROWS)

    def chip_device(k):
        tx, ty = chip(k)
        return (reg, tx * 2 + core, ty)

    def group_device(k):
        df, dy = divmod(k, ROWS)
        return (reg, lax.rem(f + df, FEATS), lax.rem(y + dy, ROWS))

    def region_device(k):
        return (lax.rem(reg + k, REGIONS), f, y)

    across = (reg, (1 - xl) * 2 + core, y)
    beside = (reg - xh + 1 - xh, (1 - xl) * 2 + core, y)

    first = xl * CHIP
    half = xl * CHIP + core * HALF
    early = 2048

    def rows_of(start, size):
        return pl.ds(pl.multiple_of(start, 128), size)

    loads = [
        pltpu.make_async_copy(omega, omegas.at[0], local.at[0]),
        pltpu.make_async_copy(phase, phases.at[0], local.at[1]),
        pltpu.make_async_copy(
            samples.at[rows_of(first, early), :], sample.at[pl.ds(0, early), :], local.at[2]
        ),
        pltpu.make_async_copy(w_in, w, local.at[3]),
        pltpu.make_async_copy(
            samples.at[rows_of(first + early, CHIP - early), :],
            sample.at[pl.ds(early, CHIP - early), :],
            local.at[4],
        ),
        pltpu.make_async_copy(u_in, u, local.at[5]),
        pltpu.make_async_copy(z_in, z, local.at[6]),
        pltpu.make_async_copy(targets.at[:, rows_of(half, HALF)], tgt, local.at[7]),
        pltpu.make_async_copy(
            member.at[pl.ds(pl.multiple_of(half // 128, 16), 16), :], mem, local.at[8]
        ),
        pltpu.make_async_copy(factors, low, local.at[9]),
    ]
    for load in loads:
        load.start()

    barrier = pltpu.get_barrier_semaphore()
    for k in range(1, FEATS * ROWS):
        pl.semaphore_signal(barrier, inc=1, device_id=group_device(k), device_id_type=MESH)
    for k in range(1, REGIONS):
        pl.semaphore_signal(barrier, inc=1, device_id=region_device(k), device_id_type=MESH)
    pl.semaphore_signal(barrier, inc=1, device_id=beside, device_id_type=MESH)

    with scope("load"):
        for load in loads[:3]:
            load.wait()

    scale = math.sqrt(2.0 / FEATURES)
    c1, c3, c5, c7 = (-scale * c for c in SINE)

    def make_rhs(side):
        turns = omegas[side].astype(F32) * (0.5 / math.pi)
        high = turns.astype(BF16)
        rest = (turns - high.astype(F32)).astype(BF16)
        for n in range(8):
            rhs[n, pl.ds(0, INPUTS), :] = high[:, n * 128 : n * 128 + 128]
            rhs[n, pl.ds(INPUTS, INPUTS), :] = rest[:, n * 128 : n * 128 + 128]

    def turns_of(row, n):
        block = sample[rows_of(row, 256), :]
        return dot(
            jnp.concatenate([block, block], axis=1),
            jnp.concatenate([rhs[2 * n], rhs[2 * n + 1]], axis=1),
        )

    def weights_of(it, side):
        return weights[it, side].reshape(OUTPUTS, BLOCK)

    def make_features(side, base, count, predicting):
        feat = feat_other if side else feat_mine
        turned = turned_other if side else turned_mine
        shift = phases[side] * (0.5 / math.pi)
        turns_next[...] = turns_of(base, 0)

        def body(i, _):
            tiles = [(m, n) for m in range(2) for n in range(4)]
            now = turns_next[...]
            total = None
            for t, (m, n) in enumerate(tiles):
                row = base + i * 512 + m * 256
                if t + 1 < len(tiles):
                    later = turns_of(base + i * 512 + tiles[t + 1][0] * 256, tiles[t + 1][1])
                else:
                    later = turns_of(base + jnp.minimum(i + 1, count - 1) * 512, 0)
                pieces = []
                for q in range(PIECES):
                    size = 256 // PIECES
                    turn = now[q * size : q * size + size] + shift[:, n * 256 : n * 256 + 256]
                    g = jnp.abs(turn - jnp.round(turn)) - 0.25
                    s = g * g
                    piece = (g * (c1 + s * (c3 + s * (c5 + s * c7)))).astype(BF16)
                    rows = pl.ds(pl.multiple_of(row + q * size, size), size)
                    feat[2 * n, rows, :] = piece[:, :128]
                    feat[2 * n + 1, rows, :] = piece[:, 128:]
                    pieces.append(piece)
                value = jnp.concatenate(pieces, axis=0).T
                cols = pl.ds(n * 256, 256)
                block = row // 128
                turned[block, cols, :] = value[:, :128]
                turned[block + 1, cols, :] = value[:, 128:]
                if predicting:
                    some = slice(n * 256, n * 256 + 256)
                    before = jnp.concatenate(
                        [turned_mine[block, cols, :], turned_mine[block + 1, cols, :]], axis=1
                    )
                    part = dot(weights_of(0, 0)[:, some], before)
                    part += dot(weights_of(0, 1)[:, some], value)
                    total = part if n == 0 else total + part
                    if n == 3:
                        pred[:, rows_of(row, 256)] = total
                now = later
            turns_next[...] = now
            return 0

        lax.fori_loop(0, count, body, 0)

    with scope("features_mine"):
        make_rhs(0)
        make_features(0, 0, early // 512, False)

    with scope("barrier"):
        pl.semaphore_wait(barrier, 31)

    om = [
        remote(
            omegas.at[0, pl.ds(0, 32), :],
            omegas.at[1, pl.ds(0, 32), :],
            om_s.at[0],
            om_r.at[0],
            across,
        ),
        remote(
            omegas.at[0, pl.ds(32, 96), :],
            omegas.at[1, pl.ds(32, 96), :],
            om_s.at[1],
            om_r.at[1],
            beside,
        ),
        remote(phases.at[0], phases.at[1], om_s.at[2], om_r.at[2], across),
    ]
    sent = []

    def start(copies, whole, send, recv):
        for copy in copies:
            copy.start()
        if send is not None:
            sent.append((whole, send, recv))

    def arrived(whole, send, recv):
        remote(whole, whole, send, recv, partner).wait_recv()

    def gather(it):
        for side, count in ((0, 3), (1, 4)):
            start(
                [
                    remote(
                        weights.at[it, 0, y],
                        weights.at[it, side, y],
                        ag_s.at[it, side],
                        ag_r.at[it, side],
                        chip_device(k),
                    )
                    for k in range(4 * side + 4 - count, 4 * side + 4)
                ],
                weights.at[it, side, pl.ds(0, count)],
                ag_s.at[it, side],
                ag_r.at[it, side],
            )

    def gather_wait(it, side):
        arrived(
            weights.at[it, side, pl.ds(0, 3 + side)], ag_s.at[it, side], ag_r.at[it, side]
        )

    def to_regions(source, buffer, it, send, recv):
        start(
            [
                remote(
                    source(lax.rem(reg + k, REGIONS)),
                    buffer.at[it, reg],
                    send.at[it],
                    recv.at[it],
                    region_device(k),
                )
                for k in range(1, REGIONS)
            ],
            buffer.at[it, pl.ds(0, REGIONS - 1)],
            send.at[it],
            recv.at[it],
        )

    def from_regions(buffer, it, send, recv):
        arrived(buffer.at[it, pl.ds(0, REGIONS - 1)], send.at[it], recv.at[it])

    def send_rho(it, rho):
        rhos[it, reg] = jnp.broadcast_to(rho, (1, 128))
        to_regions(lambda _: rhos.at[it, reg], rhos, it, ro_s, ro_r)

    loads[3].wait()
    weights[0, 0, y] = w[...].astype(BF16)
    gather(0)
    for copy in om:
        copy.start()
    rho = jnp.full((1, 1), rho_in[0], F32)
    send_rho(0, rho)

    loads[4].wait()
    with scope("features_mine_rest"):
        make_features(0, early, (CHIP - early) // 512, False)

    with scope("omega_wait"):
        for copy in om:
            copy.wait_recv()

    eye = lax.broadcasted_iota(jnp.int32, (128, 128), 0) == lax.broadcasted_iota(
        jnp.int32, (128, 128), 1
    )

    def make_inverse():
        ys, qs, columns, lanes = [], [], [], []
        inv[...] = jnp.zeros_like(inv)
        inv_t[...] = jnp.zeros_like(inv_t)
        for b in range(8):
            at = pl.ds(b * 128, 128)
            block = low[at, at]
            diagonal = jnp.where(eye, block, 0.0)
            column = 1.0 / jnp.sum(diagonal, axis=1, keepdims=True)
            lanes.append(1.0 / jnp.sum(diagonal, axis=0, keepdims=True))
            columns.append(column)
            n = jnp.where(eye, 0.0, block) * column
            ys.append(-n)
            qs.append(dot(n.astype(BF16), n.astype(BF16)))
        for step in range(6):
            for b in range(8):
                q = qs[b].astype(BF16)
                if step < 5:
                    both = dot(jnp.concatenate([ys[b].astype(BF16), q], axis=0), q)
                    ys[b] = ys[b] + qs[b] + both[:128]
                    qs[b] = both[128:]
                else:
                    ys[b] = ys[b] + qs[b] + dot(ys[b].astype(BF16), q)
        for b in range(8):
            inv[b, pl.ds(b * 128, 128), :] = ys[b].astype(BF16)

        def square(top, size):
            return jnp.concatenate(
                [inv[top // 128 + i, pl.ds(top, size), :] for i in range(size // 128)], axis=1
            )

        size = 128
        while size < BLOCK:
            for top in range(0, BLOCK, 2 * size):
                column = jnp.concatenate(
                    columns[(top + size) // 128 : (top + 2 * size) // 128], axis=0
                )
                c = low[pl.ds(top + size, size), pl.ds(top, size)] * column
                t = c + dot(square(top + size, size), c.astype(BF16))
                t = (-t - dot(t.astype(BF16), square(top, size))).astype(BF16)
                for i in range(size // 128):
                    inv[top // 128 + i, pl.ds(top + size, size), :] = t[:, i * 128 : i * 128 + 128]
            size *= 2
        for r in range(8):
            for b in range(r + 1):
                inv_t[r, pl.ds(b * 128, 128), :] = inv[b, pl.ds(r * 128, 128), :].T
        return jnp.concatenate(lanes, axis=1)

    def predict(it, side, base, count, more):
        turned = turned_other if side else turned_mine
        for m in range(count):
            rows = rows_of(base + m * 256, 256)
            block = base // 128 + 2 * m
            part = dot(
                weights_of(it, side), jnp.concatenate([turned[block], turned[block + 1]], axis=1)
            )
            pred[:, rows] = pred[:, rows] + part if more else part

    def scale_to(value, shape):
        return jnp.broadcast_to(value, shape)

    def consensus_send(it, rho):
        value = scale_to(rho, (SLICE, BLOCK)) * (w[...] + u[...])
        for k in range(REGIONS):
            r, c = divmod(k, 8)
            cons_src[it, k] = value[r * 8 : r * 8 + 8, c * 128 : c * 128 + 128]
        cons_sum[it, reg] = cons_src[it, reg]
        to_regions(lambda r: cons_src.at[it, r], cons_sum, it, cs_s, cs_r)

    def consensus_sum(it):
        with scope("sum_wait"):
            from_regions(cons_sum, it, cs_s, cs_r)
            from_regions(rhos, it, ro_s, ro_r)
        total, divisor = cons_sum[it, 0], rhos[it, 0]
        for k in range(1, REGIONS):
            total = total + cons_sum[it, k]
            divisor = divisor + rhos[it, k]
        cons_all[it, reg] = total / divisor
        to_regions(lambda _: cons_all.at[it, reg], cons_all, it, ca_s, ca_r)

    def consensus_take(it):
        with scope("take_wait"):
            from_regions(cons_all, it, ca_s, ca_r)
        gap = jnp.zeros((8, 128), F32)
        drift = jnp.zeros((8, 128), F32)
        for k in range(REGIONS):
            r, c = divmod(k, 8)
            at = (pl.ds(r * 8, 8), pl.ds(c * 128, 128))
            new = cons_all[it, k]
            apart = w[at] - new
            moved = new - z[at]
            gap += apart * apart
            drift += moved * moved
            u[at] = u[at] + apart
            z[at] = new
        row = lax.broadcasted_iota(jnp.int32, (2, 128), 0)
        gap = scale_to(jnp.sum(gap, axis=0, keepdims=True), (2, 128))
        drift = scale_to(jnp.sum(drift, axis=0, keepdims=True), (2, 128))
        me = f * ROWS + y
        gaps[it, me] = jnp.where(row == 0, gap, drift)
        start(
            [
                remote(gaps.at[it, me], gaps.at[it, me], gp_s.at[it], gp_r.at[it], group_device(k))
                for k in range(1, FEATS * ROWS)
            ],
            gaps.at[it, pl.ds(0, FEATS * ROWS - 1)],
            gp_s.at[it],
            gp_r.at[it],
        )

    def penalty(it, rho):
        with scope("gap_wait"):
            arrived(gaps.at[it, pl.ds(0, FEATS * ROWS - 1)], gp_s.at[it], gp_r.at[it])
        total = gaps[it, 0]
        for k in range(1, FEATS * ROWS):
            total = total + gaps[it, k]
        total = jnp.sum(total, axis=1, keepdims=True)
        offset = 0.01 * FEATURES * OUTPUTS
        gap, drift = total[0:1], rho * rho * total[1:2]
        new = rho * jnp.sqrt((gap + offset) / (drift + offset))
        u[...] = u[...] * scale_to(rho / new, (SLICE, BLOCK))
        pen_out[:, it : it + 1] = new
        return new

    mine_at = core * HALF
    other_at = (1 - core) * HALF
    lanes = None
    for it in range(ITERS):
        if it == 0:
            with scope("gather_wait"):
                gather_wait(0, 0)
                gather_wait(0, 1)
            with scope("features_other"):
                make_rhs(1)
                make_features(1, other_at, 4, True)
        else:
            with scope("gather_wait"):
                gather_wait(it, 0)
            with scope("predict_first"):
                predict(it, 0, 0, 16, False)
            if it > 1:
                consensus_sum(it - 1)
            with scope("gather_wait"):
                gather_wait(it, 1)
            with scope("predict_other"):
                predict(it, 1, other_at, 8, True)
        for g in range(HALF // 128):
            pred_send[it, g] = pred[:, rows_of(other_at + g * 128, 128)].astype(BF16)
        to_pair = remote(
            pred_send.at[it], pred_recv.at[it], pair_s.at[it, 0], pair_r.at[it, 0], partner
        )
        start([to_pair], pred_send.at[it], pair_s.at[it, 0], pair_r.at[it, 0])
        if it == 0:
            with scope("features_other_rest"):
                make_features(1, mine_at, 4, True)
            for load in loads[5:]:
                load.wait()
        else:
            if it == 1:
                consensus_sum(it - 1)
            with scope("predict_mine"):
                predict(it, 1, mine_at, 8, True)
        with scope("pred_wait"):
            to_pair.wait_recv()
        with scope("residual"):
            for g in range(HALF // 128):
                value = pred[:, rows_of(mine_at + g * 128, 128)] + pred_recv[it, g].astype(F32)
                value = value - tgt[:, g * 128 : g * 128 + 128].astype(F32)
                res_own[it, g] = (mem[g : g + 1, :].astype(F32) * value).astype(BF16)
        res = remote(res_own.at[it], res_other.at[it], pair_s.at[it, 1], pair_r.at[it, 1], partner)
        start([res], res_own.at[it], pair_s.at[it, 1], pair_r.at[it, 1])

        def gradient_part(residual, feat, at, n):
            rows = rows_of(at, HALF)
            return dot(
                jnp.concatenate([residual[it, g] for g in range(HALF // 128)], axis=1),
                jnp.concatenate([feat[2 * n, rows, :], feat[2 * n + 1, rows, :]], axis=1),
            )

        with scope("gradient_mine"):
            for side, feat in ((1, feat_other), (0, feat_mine)):
                for n in range(4):
                    acc[side, :, pl.ds(n * 256, 256)] = gradient_part(res_own, feat, mine_at, n)
        with scope("res_wait"):
            res.wait_recv()
        for side, feat in ((1, feat_other), (0, feat_mine)):
            for part in range(2):
                with scope("gradient_other"):
                    for n in range(2 * part, 2 * part + 2):
                        cols = pl.ds(n * 256, 256)
                        total = acc[side, :, cols] + gradient_part(res_other, feat, other_at, n)
                        grad_send[it, side, :, :, cols] = total.reshape(ROWS, SLICE, 256).astype(BF16)
                cols = pl.ds(part * 512, 512)
                start(
                    [
                        remote(
                            grad_send.at[it, side, chip(k)[1], :, cols],
                            grad_recv.at[it, k, :, cols],
                            rs_s.at[it],
                            rs_r.at[it],
                            chip_device(k),
                        )
                        for k in range(side * 4, side * 4 + 4)
                        if k
                    ],
                    grad_recv.at[it, pl.ds(1, 7)],
                    rs_s.at[it] if side == 0 and part == 1 else None,
                    rs_r.at[it],
                )
        if it == 0:
            with scope("inverse"):
                lanes = make_inverse()
        else:
            consensus_take(it - 1)
        old_rho_u = scale_to(rho, (SLICE, BLOCK)) * u[...]
        gradient = grad_send[it, 0, y].astype(F32)
        with scope("grad_wait"):
            arrived(grad_recv.at[it, pl.ds(1, 7)], rs_s.at[it], rs_r.at[it])
        with scope("solve"):
            for k in range(1, 8):
                gradient = gradient + grad_recv[it, k].astype(F32)
            right = jnp.concatenate([gradient + old_rho_u, w[...] - z[...]], axis=0) * lanes
            low16 = right.astype(BF16)
            right = right + jnp.concatenate(
                [
                    dot(
                        low16[:, : n * 256 + 256],
                        jnp.concatenate(
                            [inv_t[2 * n + i, pl.ds(0, n * 256 + 256), :] for i in range(2)], axis=1
                        ),
                    )
                    for n in range(4)
                ],
                axis=1,
            )
            low16 = right.astype(BF16)
            right = right + jnp.concatenate(
                [
                    dot(
                        low16[:, n * 256 :],
                        jnp.concatenate(
                            [
                                inv[2 * n + i, pl.ds(n * 256, BLOCK - n * 256), :]
                                for i in range(2)
                            ],
                            axis=1,
                        ),
                    )
                    for n in range(4)
                ],
                axis=1,
            )
            right = right * lanes
        if it:
            rho = penalty(it - 1, rho)
        new = w[...] - right[:SLICE] - scale_to(rho, (SLICE, BLOCK)) * right[SLICE:]
        w[...] = new
        with scope("consensus_send"):
            consensus_send(it, rho)
        if it < ITERS - 1:
            weights[it + 1, 0, y] = new.astype(BF16)
            gather(it + 1)
        if it:
            send_rho(it, rho)

    consensus_sum(ITERS - 1)
    consensus_take(ITERS - 1)
    penalty(ITERS - 1, rho)
    for copy in om:
        copy.wait_send()
    for whole, send, recv in sent:
        remote(whole, whole, send, recv, partner).wait_send()


def hand_over(*refs):
    for source, out in zip(refs[:4], refs[4:]):
        out[...] = source[...]


def per_device(
    samples,
    targets,
    member,
    omega,
    phase,
    factors,
    weights_init,
    duals_init,
    consensus_init,
    penalty_init,
):
    hbm = pl.BlockSpec(memory_space=pl.ANY)
    vmem = pl.BlockSpec(memory_space=pltpu.VMEM)
    smem = pl.BlockSpec(memory_space=pltpu.SMEM)
    state = jax.ShapeDtypeStruct((SLICE, BLOCK), F32)
    dma = pltpu.SemaphoreType.DMA
    w, u, z, pen = pl.pallas_call(
        kernel,
        out_shape=(state, state, state, jax.ShapeDtypeStruct((1, ITERS), F32)),
        in_specs=[hbm] * 9 + [smem],
        out_specs=(vmem,) * 4,
        scratch_shapes=[
            pltpu.VMEM((8, CHIP, 128), BF16),
            pltpu.VMEM((8, CHIP, 128), BF16),
            pltpu.VMEM((CHIP // 128, BLOCK, 128), BF16),
            pltpu.VMEM((CHIP // 128, BLOCK, 128), BF16),
            pltpu.VMEM((CHIP, INPUTS), BF16),
            pltpu.VMEM((2, INPUTS, BLOCK), BF16),
            pltpu.VMEM((2, 1, BLOCK), F32),
            pltpu.VMEM((8, 2 * INPUTS, 128), BF16),
            pltpu.VMEM((256, 256), F32),
            pltpu.VMEM((OUTPUTS, HALF), BF16),
            pltpu.VMEM((16, 128), jnp.int32),
            pltpu.VMEM((BLOCK, BLOCK), F32),
            pltpu.VMEM((8, BLOCK, 128), BF16),
            pltpu.VMEM((8, BLOCK, 128), BF16),
            pltpu.VMEM((ITERS, 2, ROWS, SLICE, BLOCK), BF16),
            pltpu.VMEM((OUTPUTS, CHIP), F32),
            pltpu.VMEM((ITERS, 16, OUTPUTS, 128), BF16),
            pltpu.VMEM((ITERS, 16, OUTPUTS, 128), BF16),
            pltpu.VMEM((ITERS, 16, OUTPUTS, 128), BF16),
            pltpu.VMEM((ITERS, 16, OUTPUTS, 128), BF16),
            pltpu.VMEM((2, OUTPUTS, BLOCK), F32),
            pltpu.VMEM((ITERS, 2, ROWS, SLICE, BLOCK), BF16),
            pltpu.VMEM((ITERS, 8, SLICE, BLOCK), BF16),
            pltpu.VMEM((ITERS, REGIONS, 8, 128), F32),
            pltpu.VMEM((ITERS, REGIONS, 8, 128), F32),
            pltpu.VMEM((ITERS, REGIONS, 8, 128), F32),
            pltpu.VMEM((ITERS, REGIONS, 1, 128), F32),
            pltpu.VMEM((ITERS, FEATS * ROWS, 2, 128), F32),
            dma((10,)),
            dma((3,)),
            dma((3,)),
            dma((ITERS, 2)),
            dma((ITERS, 2)),
            dma((ITERS,)),
            dma((ITERS,)),
            dma((ITERS, 2)),
            dma((ITERS, 2)),
            dma((ITERS,)),
            dma((ITERS,)),
            dma((ITERS,)),
            dma((ITERS,)),
            dma((ITERS,)),
            dma((ITERS,)),
            dma((ITERS,)),
            dma((ITERS,)),
        ],
        compiler_params=pltpu.CompilerParams(
            collective_id=0, has_side_effects=True, vmem_limit_bytes=60 * 1024 * 1024
        ),
        name="admm",
    )(
        samples,
        targets.T,
        member.reshape(64, 128),
        omega,
        phase.reshape(1, BLOCK),
        factors,
        weights_init.T,
        duals_init.T,
        consensus_init.T,
        penalty_init,
    )
    w, u, z, pen = pl.pallas_call(
        hand_over,
        out_shape=(state, state, state, jax.ShapeDtypeStruct((1, ITERS), F32)),
        in_specs=[vmem] * 4,
        out_specs=(vmem,) * 4,
        name="hand_over",
    )(w, u, z, pen)
    return w.T, u.T, z.T, pen


def solution(mesh):
    return jax.shard_map(
        per_device,
        mesh=mesh,
        in_specs=(
            P(("region", "row"), None),
            P(("region", "row"), None),
            P(("region", "row")),
            P(None, "feat"),
            P("feat"),
            P(("region", "feat"), None),
            P(("region", "feat"), "row"),
            P(("region", "feat"), "row"),
            P("feat", "row"),
            P("region"),
        ),
        out_specs=(
            P(("region", "feat"), "row"),
            P(("region", "feat"), "row"),
            P("feat", "row"),
            P("region", None),
        ),
        check_vma=False,
    )
```

```python
import math

import jax
import jax.numpy as jnp
from jax import lax
from jax.experimental import pallas as pl
from jax.experimental.pallas import tpu as pltpu
from jax.sharding import PartitionSpec as P

FEATURES = 4096
OUTPUTS = 64
ITERS = 3
REGIONS = 16
ROWS = 4
FEATS = 4
BLOCK = 1024
INPUTS = 128
CHIP = 4096
HALF = 2048
SLICE = 16
MESH = pl.DeviceIdType.MESH
F32 = jnp.float32
BF16 = jnp.bfloat16
SINE = (6.281280070289077, -41.095242279919105, 73.58550951045723)
PIECES = 4
NT = (((1,), (1,)), ((), ()))
scope = jax.named_scope


def dot(a, b):
    return jnp.dot(a, b, preferred_element_type=F32)


def dot_nt(a, b):
    return lax.dot_general(a, b, NT, preferred_element_type=F32)


def remote(src, dst, send, recv, device):
    return pltpu.make_async_remote_copy(
        src_ref=src,
        dst_ref=dst,
        send_sem=send,
        recv_sem=recv,
        device_id=device,
        device_id_type=MESH,
    )


def kernel(
    samples,
    targets,
    member,
    omega,
    phase,
    factors,
    w_in,
    u_in,
    z_in,
    rho_in,
    w,
    u,
    z,
    pen_out,
    feat_mine,
    feat_other,
    turned_mine,
    turned_other,
    sample,
    omegas,
    phases,
    rhs,
    turns_next,
    tgt,
    mem,
    low,
    inv,
    inv_t,
    weights,
    pred,
    pred_send,
    pred_recv,
    res_own,
    res_other,
    acc,
    grad_send,
    grad_recv,
    cons_src,
    cons_sum,
    cons_all,
    rhos,
    gaps,
    local,
    om_s,
    om_r,
    ag_s,
    ag_r,
    rs_s,
    rs_r,
    pair_s,
    pair_r,
    cs_s,
    cs_r,
    ca_s,
    ca_r,
    gp_s,
    gp_r,
    ro_s,
    ro_r,
):
    reg = lax.axis_index("region")
    f = lax.axis_index("feat")
    y = lax.axis_index("row")
    core = lax.rem(f, 2)
    xl = f // 2
    xh = lax.rem(reg, 2)
    partner = (reg, xl * 2 + 1 - core, y)

    def chip(k):
        dx, dy = divmod(k, ROWS)
        return lax.rem(xl + dx, 2), lax.rem(y + dy, ROWS)

    def chip_device(k):
        tx, ty = chip(k)
        return (reg, tx * 2 + core, ty)

    def group_device(k):
        df, dy = divmod(k, ROWS)
        return (reg, lax.rem(f + df, FEATS), lax.rem(y + dy, ROWS))

    def region_device(k):
        return (lax.rem(reg + k, REGIONS), f, y)

    across = (reg, (1 - xl) * 2 + core, y)
    beside = (reg - xh + 1 - xh, (1 - xl) * 2 + core, y)

    first = xl * CHIP
    half = xl * CHIP + core * HALF
    early = 2048

    def rows_of(start, size):
        return pl.ds(pl.multiple_of(start, 128), size)

    loads = [
        pltpu.make_async_copy(omega, omegas.at[0], local.at[0]),
        pltpu.make_async_copy(phase, phases.at[0], local.at[1]),
        pltpu.make_async_copy(
            samples.at[rows_of(first, early), :], sample.at[pl.ds(0, early), :], local.at[2]
        ),
        pltpu.make_async_copy(w_in, w, local.at[3]),
        pltpu.make_async_copy(
            samples.at[rows_of(first + early, CHIP - early), :],
            sample.at[pl.ds(early, CHIP - early), :],
            local.at[4],
        ),
        pltpu.make_async_copy(u_in, u, local.at[5]),
        pltpu.make_async_copy(z_in, z, local.at[6]),
        pltpu.make_async_copy(targets.at[:, rows_of(half, HALF)], tgt, local.at[7]),
        pltpu.make_async_copy(
            member.at[pl.ds(pl.multiple_of(half // 128, 16), 16), :], mem, local.at[8]
        ),
        pltpu.make_async_copy(factors, low, local.at[9]),
    ]
    for load in loads:
        load.start()

    barrier = pltpu.get_barrier_semaphore()
    for k in range(1, FEATS * ROWS):
        pl.semaphore_signal(barrier, inc=1, device_id=group_device(k), device_id_type=MESH)
    for k in range(1, REGIONS):
        pl.semaphore_signal(barrier, inc=1, device_id=region_device(k), device_id_type=MESH)
    pl.semaphore_signal(barrier, inc=1, device_id=beside, device_id_type=MESH)

    with scope("load"):
        for load in loads[:3]:
            load.wait()

    scale = math.sqrt(2.0 / FEATURES)
    c1, c3, c5 = (-scale * c for c in SINE)

    def make_rhs(side):
        turns = omegas[side].astype(F32) * (0.5 / math.pi)
        high = turns.astype(BF16)
        rest = (turns - high.astype(F32)).astype(BF16)
        for n in range(8):
            rhs[n, pl.ds(0, INPUTS), :] = high[:, n * 128 : n * 128 + 128]
            rhs[n, pl.ds(INPUTS, INPUTS), :] = rest[:, n * 128 : n * 128 + 128]

    def turns_of(row, n):
        block = sample[rows_of(row, 256), :]
        return dot(
            jnp.concatenate([block, block], axis=1),
            jnp.concatenate([rhs[2 * n], rhs[2 * n + 1]], axis=1),
        )

    def weights_of(it, side):
        return weights[it, side].reshape(OUTPUTS, BLOCK)

    def make_features(side, base, count, predicting):
        feat = feat_other if side else feat_mine
        turned = turned_other if side else turned_mine
        shift = phases[side] * (0.5 / math.pi)
        turns_next[...] = turns_of(base, 0)

        def body(i, _):
            tiles = [(m, n) for m in range(2) for n in range(4)]
            now = turns_next[...]
            total = None
            for t, (m, n) in enumerate(tiles):
                row = base + i * 512 + m * 256
                if t + 1 < len(tiles):
                    later = turns_of(base + i * 512 + tiles[t + 1][0] * 256, tiles[t + 1][1])
                else:
                    later = turns_of(base + jnp.minimum(i + 1, count - 1) * 512, 0)
                pieces = []
                for q in range(PIECES):
                    size = 256 // PIECES
                    turn = now[q * size : q * size + size] + shift[:, n * 256 : n * 256 + 256]
                    g = jnp.abs(turn - jnp.round(turn)) - 0.25
                    s = g * g
                    piece = (g * (c1 + s * (c3 + s * c5))).astype(BF16)
                    rows = pl.ds(pl.multiple_of(row + q * size, size), size)
                    feat[2 * n, rows, :] = piece[:, :128]
                    feat[2 * n + 1, rows, :] = piece[:, 128:]
                    pieces.append(piece)
                value = jnp.concatenate(pieces, axis=0).T
                cols = pl.ds(n * 256, 256)
                block = row // 128
                turned[block, cols, :] = value[:, :128]
                turned[block + 1, cols, :] = value[:, 128:]
                if predicting:
                    some = slice(n * 256, n * 256 + 256)
                    before = jnp.concatenate(
                        [turned_mine[block, cols, :], turned_mine[block + 1, cols, :]], axis=1
                    )
                    part = dot(weights_of(0, 0)[:, some], before)
                    part += dot(weights_of(0, 1)[:, some], value)
                    total = part if n == 0 else total + part
                    if n == 3:
                        pred[:, rows_of(row, 256)] = total
                now = later
            turns_next[...] = now
            return 0

        lax.fori_loop(0, count, body, 0)

    with scope("features_mine"):
        make_rhs(0)
        make_features(0, 0, early // 512, False)

    with scope("barrier"):
        pl.semaphore_wait(barrier, 31)

    om = [
        remote(
            omegas.at[0, pl.ds(0, 32), :],
            omegas.at[1, pl.ds(0, 32), :],
            om_s.at[0],
            om_r.at[0],
            across,
        ),
        remote(
            omegas.at[0, pl.ds(32, 96), :],
            omegas.at[1, pl.ds(32, 96), :],
            om_s.at[1],
            om_r.at[1],
            beside,
        ),
        remote(phases.at[0], phases.at[1], om_s.at[2], om_r.at[2], across),
    ]
    sent = []

    def start(copies, whole, send, recv):
        for copy in copies:
            copy.start()
        if send is not None:
            sent.append((whole, send, recv))

    def arrived(whole, send, recv):
        remote(whole, whole, send, recv, partner).wait_recv()

    def gather(it):
        for side, count in ((0, 3), (1, 4)):
            start(
                [
                    remote(
                        weights.at[it, 0, y],
                        weights.at[it, side, y],
                        ag_s.at[it, side],
                        ag_r.at[it, side],
                        chip_device(k),
                    )
                    for k in range(4 * side + 4 - count, 4 * side + 4)
                ],
                weights.at[it, side, pl.ds(0, count)],
                ag_s.at[it, side],
                ag_r.at[it, side],
            )

    def gather_wait(it, side):
        arrived(
            weights.at[it, side, pl.ds(0, 3 + side)], ag_s.at[it, side], ag_r.at[it, side]
        )

    def to_regions(source, buffer, it, send, recv):
        start(
            [
                remote(
                    source(lax.rem(reg + k, REGIONS)),
                    buffer.at[it, reg],
                    send.at[it],
                    recv.at[it],
                    region_device(k),
                )
                for k in range(1, REGIONS)
            ],
            buffer.at[it, pl.ds(0, REGIONS - 1)],
            send.at[it],
            recv.at[it],
        )

    def from_regions(buffer, it, send, recv):
        arrived(buffer.at[it, pl.ds(0, REGIONS - 1)], send.at[it], recv.at[it])

    def send_rho(it, rho):
        rhos[it, reg] = jnp.broadcast_to(rho, (1, 128))
        to_regions(lambda _: rhos.at[it, reg], rhos, it, ro_s, ro_r)

    loads[3].wait()
    weights[0, 0, y] = w[...].astype(BF16)
    gather(0)
    for copy in om:
        copy.start()
    rho = jnp.full((1, 1), rho_in[0], F32)
    send_rho(0, rho)

    loads[4].wait()
    with scope("features_mine_rest"):
        make_features(0, early, (CHIP - early) // 512, False)

    with scope("omega_wait"):
        for copy in om:
            copy.wait_recv()

    eye = lax.broadcasted_iota(jnp.int32, (128, 128), 0) == lax.broadcasted_iota(
        jnp.int32, (128, 128), 1
    )

    def make_inverse():
        ys, qs, columns, lanes = [], [], [], []
        inv[...] = jnp.zeros_like(inv)
        inv_t[...] = jnp.zeros_like(inv_t)
        for b in range(8):
            at = pl.ds(b * 128, 128)
            block = low[at, at]
            diagonal = jnp.where(eye, block, 0.0)
            column = 1.0 / jnp.sum(diagonal, axis=1, keepdims=True)
            lanes.append(1.0 / jnp.sum(diagonal, axis=0, keepdims=True))
            columns.append(column)
            n = jnp.where(eye, 0.0, block) * column
            ys.append(-n)
            qs.append(dot(n.astype(BF16), n.astype(BF16)))
        for step in range(6):
            for b in range(8):
                q = qs[b].astype(BF16)
                if step < 5:
                    both = dot(jnp.concatenate([ys[b].astype(BF16), q], axis=0), q)
                    ys[b] = ys[b] + qs[b] + both[:128]
                    qs[b] = both[128:]
                else:
                    ys[b] = ys[b] + qs[b] + dot(ys[b].astype(BF16), q)
        for b in range(8):
            inv[b, pl.ds(b * 128, 128), :] = ys[b].astype(BF16)

        def square(top, size):
            return jnp.concatenate(
                [inv[top // 128 + i, pl.ds(top, size), :] for i in range(size // 128)], axis=1
            )

        size = 128
        while size < BLOCK:
            for top in range(0, BLOCK, 2 * size):
                column = jnp.concatenate(
                    columns[(top + size) // 128 : (top + 2 * size) // 128], axis=0
                )
                c = low[pl.ds(top + size, size), pl.ds(top, size)] * column
                t = c + dot(square(top + size, size), c.astype(BF16))
                t = (-t - dot(t.astype(BF16), square(top, size))).astype(BF16)
                for i in range(size // 128):
                    inv[top // 128 + i, pl.ds(top + size, size), :] = t[:, i * 128 : i * 128 + 128]
            size *= 2
        for r in range(8):
            for b in range(r + 1):
                inv_t[r, pl.ds(b * 128, 128), :] = inv[b, pl.ds(r * 128, 128), :].T
        return jnp.concatenate(lanes, axis=1)

    def predict(it, side, base, count, more):
        turned = turned_other if side else turned_mine
        for m in range(count):
            rows = rows_of(base + m * 256, 256)
            block = base // 128 + 2 * m
            part = dot(
                weights_of(it, side), jnp.concatenate([turned[block], turned[block + 1]], axis=1)
            )
            pred[:, rows] = pred[:, rows] + part if more else part

    def scale_to(value, shape):
        return jnp.broadcast_to(value, shape)

    def consensus_send(it, rho):
        value = scale_to(rho, (SLICE, BLOCK)) * (w[...] + u[...])
        for k in range(REGIONS):
            r, c = divmod(k, 8)
            cons_src[it, k] = value[r * 8 : r * 8 + 8, c * 128 : c * 128 + 128]
        cons_sum[it, reg] = cons_src[it, reg]
        to_regions(lambda r: cons_src.at[it, r], cons_sum, it, cs_s, cs_r)

    def consensus_sum(it):
        with scope("sum_wait"):
            from_regions(cons_sum, it, cs_s, cs_r)
            from_regions(rhos, it, ro_s, ro_r)
        total, divisor = cons_sum[it, 0], rhos[it, 0]
        for k in range(1, REGIONS):
            total = total + cons_sum[it, k]
            divisor = divisor + rhos[it, k]
        cons_all[it, reg] = total / divisor
        to_regions(lambda _: cons_all.at[it, reg], cons_all, it, ca_s, ca_r)

    def consensus_take(it):
        with scope("take_wait"):
            from_regions(cons_all, it, ca_s, ca_r)
        gap = jnp.zeros((8, 128), F32)
        drift = jnp.zeros((8, 128), F32)
        for k in range(REGIONS):
            r, c = divmod(k, 8)
            at = (pl.ds(r * 8, 8), pl.ds(c * 128, 128))
            new = cons_all[it, k]
            apart = w[at] - new
            moved = new - z[at]
            gap += apart * apart
            drift += moved * moved
            u[at] = u[at] + apart
            z[at] = new
        row = lax.broadcasted_iota(jnp.int32, (2, 128), 0)
        gap = scale_to(jnp.sum(gap, axis=0, keepdims=True), (2, 128))
        drift = scale_to(jnp.sum(drift, axis=0, keepdims=True), (2, 128))
        me = f * ROWS + y
        gaps[it, me] = jnp.where(row == 0, gap, drift)
        start(
            [
                remote(gaps.at[it, me], gaps.at[it, me], gp_s.at[it], gp_r.at[it], group_device(k))
                for k in range(1, FEATS * ROWS)
            ],
            gaps.at[it, pl.ds(0, FEATS * ROWS - 1)],
            gp_s.at[it],
            gp_r.at[it],
        )

    def penalty(it, rho):
        with scope("gap_wait"):
            arrived(gaps.at[it, pl.ds(0, FEATS * ROWS - 1)], gp_s.at[it], gp_r.at[it])
        total = gaps[it, 0]
        for k in range(1, FEATS * ROWS):
            total = total + gaps[it, k]
        total = jnp.sum(total, axis=1, keepdims=True)
        offset = 0.01 * FEATURES * OUTPUTS
        gap, drift = total[0:1], rho * rho * total[1:2]
        new = rho * jnp.sqrt((gap + offset) / (drift + offset))
        u[...] = u[...] * scale_to(rho / new, (SLICE, BLOCK))
        pen_out[:, it : it + 1] = new
        return new

    mine_at = core * HALF
    other_at = (1 - core) * HALF
    lanes = None
    for it in range(ITERS):
        if it == 0:
            with scope("gather_wait"):
                gather_wait(0, 0)
                gather_wait(0, 1)
            with scope("features_other"):
                make_rhs(1)
                make_features(1, other_at, 4, True)
        else:
            with scope("gather_wait"):
                gather_wait(it, 0)
            with scope("predict_first"):
                predict(it, 0, 0, 16, False)
            if it > 1:
                consensus_sum(it - 1)
            with scope("gather_wait"):
                gather_wait(it, 1)
            with scope("predict_other"):
                predict(it, 1, other_at, 8, True)
        for g in range(HALF // 128):
            pred_send[it, g] = pred[:, rows_of(other_at + g * 128, 128)].astype(BF16)
        to_pair = remote(
            pred_send.at[it], pred_recv.at[it], pair_s.at[it, 0], pair_r.at[it, 0], partner
        )
        start([to_pair], pred_send.at[it], pair_s.at[it, 0], pair_r.at[it, 0])
        if it == 0:
            with scope("features_other_rest"):
                make_features(1, mine_at, 4, True)
            for load in loads[5:]:
                load.wait()
        else:
            if it == 1:
                consensus_sum(it - 1)
            with scope("predict_mine"):
                predict(it, 1, mine_at, 8, True)
        with scope("pred_wait"):
            to_pair.wait_recv()
        with scope("residual"):
            for g in range(HALF // 128):
                value = pred[:, rows_of(mine_at + g * 128, 128)] + pred_recv[it, g].astype(F32)
                value = value - tgt[:, g * 128 : g * 128 + 128].astype(F32)
                res_own[it, g] = (mem[g : g + 1, :].astype(F32) * value).astype(BF16)
        res = remote(res_own.at[it], res_other.at[it], pair_s.at[it, 1], pair_r.at[it, 1], partner)
        start([res], res_own.at[it], pair_s.at[it, 1], pair_r.at[it, 1])

        def gradient_part(residual, feat, at, n):
            rows = rows_of(at, HALF)
            return dot(
                jnp.concatenate([residual[it, g] for g in range(HALF // 128)], axis=1),
                jnp.concatenate([feat[2 * n, rows, :], feat[2 * n + 1, rows, :]], axis=1),
            )

        with scope("gradient_mine"):
            for side, feat in ((1, feat_other), (0, feat_mine)):
                for n in range(4):
                    acc[side, :, pl.ds(n * 256, 256)] = gradient_part(res_own, feat, mine_at, n)
        with scope("res_wait"):
            res.wait_recv()
        for side, feat in ((1, feat_other), (0, feat_mine)):
            for part in range(2):
                with scope("gradient_other"):
                    for n in range(2 * part, 2 * part + 2):
                        cols = pl.ds(n * 256, 256)
                        total = acc[side, :, cols] + gradient_part(res_other, feat, other_at, n)
                        grad_send[it, side, :, :, cols] = total.reshape(ROWS, SLICE, 256).astype(BF16)
                cols = pl.ds(part * 512, 512)
                start(
                    [
                        remote(
                            grad_send.at[it, side, chip(k)[1], :, cols],
                            grad_recv.at[it, k, :, cols],
                            rs_s.at[it],
                            rs_r.at[it],
                            chip_device(k),
                        )
                        for k in range(side * 4, side * 4 + 4)
                        if k
                    ],
                    grad_recv.at[it, pl.ds(1, 7)],
                    rs_s.at[it] if side == 0 and part == 1 else None,
                    rs_r.at[it],
                )
        if it == 0:
            with scope("inverse"):
                lanes = make_inverse()
        else:
            consensus_take(it - 1)
        old_rho_u = scale_to(rho, (SLICE, BLOCK)) * u[...]
        gradient = grad_send[it, 0, y].astype(F32)
        with scope("grad_wait"):
            arrived(grad_recv.at[it, pl.ds(1, 7)], rs_s.at[it], rs_r.at[it])
        with scope("solve"):
            for k in range(1, 8):
                gradient = gradient + grad_recv[it, k].astype(F32)
            right = jnp.concatenate([gradient + old_rho_u, w[...] - z[...]], axis=0) * lanes
            low16 = right.astype(BF16)
            right = right + jnp.concatenate(
                [
                    dot(
                        low16[:, : n * 256 + 256],
                        jnp.concatenate(
                            [inv_t[2 * n + i, pl.ds(0, n * 256 + 256), :] for i in range(2)], axis=1
                        ),
                    )
                    for n in range(4)
                ],
                axis=1,
            )
            low16 = right.astype(BF16)
            right = right + jnp.concatenate(
                [
                    dot(
                        low16[:, n * 256 :],
                        jnp.concatenate(
                            [
                                inv[2 * n + i, pl.ds(n * 256, BLOCK - n * 256), :]
                                for i in range(2)
                            ],
                            axis=1,
                        ),
                    )
                    for n in range(4)
                ],
                axis=1,
            )
            right = right * lanes
        if it:
            rho = penalty(it - 1, rho)
        new = w[...] - right[:SLICE] - scale_to(rho, (SLICE, BLOCK)) * right[SLICE:]
        w[...] = new
        with scope("consensus_send"):
            consensus_send(it, rho)
        if it < ITERS - 1:
            weights[it + 1, 0, y] = new.astype(BF16)
            gather(it + 1)
        if it:
            send_rho(it, rho)

    consensus_sum(ITERS - 1)
    consensus_take(ITERS - 1)
    penalty(ITERS - 1, rho)
    for copy in om:
        copy.wait_send()
    for whole, send, recv in sent:
        remote(whole, whole, send, recv, partner).wait_send()


def hand_over(*refs):
    for source, out in zip(refs[:4], refs[4:]):
        out[...] = source[...]


def per_device(
    samples,
    targets,
    member,
    omega,
    phase,
    factors,
    weights_init,
    duals_init,
    consensus_init,
    penalty_init,
):
    hbm = pl.BlockSpec(memory_space=pl.ANY)
    vmem = pl.BlockSpec(memory_space=pltpu.VMEM)
    smem = pl.BlockSpec(memory_space=pltpu.SMEM)
    state = jax.ShapeDtypeStruct((SLICE, BLOCK), F32)
    dma = pltpu.SemaphoreType.DMA
    w, u, z, pen = pl.pallas_call(
        kernel,
        out_shape=(state, state, state, jax.ShapeDtypeStruct((1, ITERS), F32)),
        in_specs=[hbm] * 9 + [smem],
        out_specs=(vmem,) * 4,
        scratch_shapes=[
            pltpu.VMEM((8, CHIP, 128), BF16),
            pltpu.VMEM((8, CHIP, 128), BF16),
            pltpu.VMEM((CHIP // 128, BLOCK, 128), BF16),
            pltpu.VMEM((CHIP // 128, BLOCK, 128), BF16),
            pltpu.VMEM((CHIP, INPUTS), BF16),
            pltpu.VMEM((2, INPUTS, BLOCK), BF16),
            pltpu.VMEM((2, 1, BLOCK), F32),
            pltpu.VMEM((8, 2 * INPUTS, 128), BF16),
            pltpu.VMEM((256, 256), F32),
            pltpu.VMEM((OUTPUTS, HALF), BF16),
            pltpu.VMEM((16, 128), jnp.int32),
            pltpu.VMEM((BLOCK, BLOCK), F32),
            pltpu.VMEM((8, BLOCK, 128), BF16),
            pltpu.VMEM((8, BLOCK, 128), BF16),
            pltpu.VMEM((ITERS, 2, ROWS, SLICE, BLOCK), BF16),
            pltpu.VMEM((OUTPUTS, CHIP), F32),
            pltpu.VMEM((ITERS, 16, OUTPUTS, 128), BF16),
            pltpu.VMEM((ITERS, 16, OUTPUTS, 128), BF16),
            pltpu.VMEM((ITERS, 16, OUTPUTS, 128), BF16),
            pltpu.VMEM((ITERS, 16, OUTPUTS, 128), BF16),
            pltpu.VMEM((2, OUTPUTS, BLOCK), F32),
            pltpu.VMEM((ITERS, 2, ROWS, SLICE, BLOCK), BF16),
            pltpu.VMEM((ITERS, 8, SLICE, BLOCK), BF16),
            pltpu.VMEM((ITERS, REGIONS, 8, 128), F32),
            pltpu.VMEM((ITERS, REGIONS, 8, 128), F32),
            pltpu.VMEM((ITERS, REGIONS, 8, 128), F32),
            pltpu.VMEM((ITERS, REGIONS, 1, 128), F32),
            pltpu.VMEM((ITERS, FEATS * ROWS, 2, 128), F32),
            dma((10,)),
            dma((3,)),
            dma((3,)),
            dma((ITERS, 2)),
            dma((ITERS, 2)),
            dma((ITERS,)),
            dma((ITERS,)),
            dma((ITERS, 2)),
            dma((ITERS, 2)),
            dma((ITERS,)),
            dma((ITERS,)),
            dma((ITERS,)),
            dma((ITERS,)),
            dma((ITERS,)),
            dma((ITERS,)),
            dma((ITERS,)),
            dma((ITERS,)),
        ],
        compiler_params=pltpu.CompilerParams(
            collective_id=0, has_side_effects=True, vmem_limit_bytes=60 * 1024 * 1024
        ),
        name="admm",
    )(
        samples,
        targets.T,
        member.reshape(64, 128),
        omega,
        phase.reshape(1, BLOCK),
        factors,
        weights_init.T,
        duals_init.T,
        consensus_init.T,
        penalty_init,
    )
    w, u, z, pen = pl.pallas_call(
        hand_over,
        out_shape=(state, state, state, jax.ShapeDtypeStruct((1, ITERS), F32)),
        in_specs=[vmem] * 4,
        out_specs=(vmem,) * 4,
        name="hand_over",
    )(w, u, z, pen)
    return w.T, u.T, z.T, pen


def solution(mesh):
    return jax.shard_map(
        per_device,
        mesh=mesh,
        in_specs=(
            P(("region", "row"), None),
            P(("region", "row"), None),
            P(("region", "row")),
            P(None, "feat"),
            P("feat"),
            P(("region", "feat"), None),
            P(("region", "feat"), "row"),
            P(("region", "feat"), "row"),
            P("feat", "row"),
            P("region"),
        ),
        out_specs=(
            P(("region", "feat"), "row"),
            P(("region", "feat"), "row"),
            P("feat", "row"),
            P("region", None),
        ),
        check_vma=False,
    )
```

```python
import math

import jax
import jax.numpy as jnp
from jax import lax
from jax.experimental import pallas as pl
from jax.experimental.pallas import tpu as pltpu
from jax.sharding import PartitionSpec as P

FEATURES = 4096
OUTPUTS = 64
ITERS = 3
REGIONS = 16
ROWS = 4
FEATS = 4
BLOCK = 1024
INPUTS = 128
CHIP = 4096
HALF = 2048
SLICE = 16
MESH = pl.DeviceIdType.MESH
F32 = jnp.float32
BF16 = jnp.bfloat16
SINE = (6.281280070289077, -41.095242279919105, 73.58550951045723)
PIECES = 4
FAR_REGIONS = sorted(range(1, REGIONS), key=lambda k: -2 * (min(k, REGIONS - k) // 2) - 3 * (k % 2))
FAR_GROUP = sorted(
    range(1, FEATS * ROWS), key=lambda k: -min(k % ROWS, ROWS - k % ROWS) - (k // ROWS in (1, 2, 3))
)
FAR_CHIPS = ((2, 1, 3), (6, 5, 7, 4))
NT = (((1,), (1,)), ((), ()))
scope = jax.named_scope


def dot(a, b):
    return jnp.dot(a, b, preferred_element_type=F32)


def dot_nt(a, b):
    return lax.dot_general(a, b, NT, preferred_element_type=F32)


def remote(src, dst, send, recv, device):
    return pltpu.make_async_remote_copy(
        src_ref=src,
        dst_ref=dst,
        send_sem=send,
        recv_sem=recv,
        device_id=device,
        device_id_type=MESH,
    )


def kernel(
    samples,
    targets,
    member,
    omega,
    phase,
    factors,
    w_in,
    u_in,
    z_in,
    rho_in,
    w,
    u,
    z,
    pen_out,
    feat_mine,
    feat_other,
    turned_mine,
    turned_other,
    sample,
    omegas,
    phases,
    rhs,
    turns_next,
    tgt,
    mem,
    low,
    inv,
    inv_t,
    weights,
    pred,
    pred_send,
    pred_recv,
    res_own,
    res_other,
    acc,
    grad_send,
    grad_recv,
    cons_src,
    cons_sum,
    cons_all,
    rhos,
    gaps,
    local,
    om_s,
    om_r,
    ag_s,
    ag_r,
    rs_s,
    rs_r,
    pair_s,
    pair_r,
    cs_s,
    cs_r,
    ca_s,
    ca_r,
    gp_s,
    gp_r,
    ro_s,
    ro_r,
):
    reg = lax.axis_index("region")
    f = lax.axis_index("feat")
    y = lax.axis_index("row")
    core = lax.rem(f, 2)
    xl = f // 2
    xh = lax.rem(reg, 2)
    partner = (reg, xl * 2 + 1 - core, y)

    def chip(k):
        dx, dy = divmod(k, ROWS)
        return lax.rem(xl + dx, 2), lax.rem(y + dy, ROWS)

    def chip_device(k):
        tx, ty = chip(k)
        return (reg, tx * 2 + core, ty)

    def group_device(k):
        df, dy = divmod(k, ROWS)
        return (reg, lax.rem(f + df, FEATS), lax.rem(y + dy, ROWS))

    def region_device(k):
        return (lax.rem(reg + k, REGIONS), f, y)

    across = (reg, (1 - xl) * 2 + core, y)
    beside = (reg - xh + 1 - xh, (1 - xl) * 2 + core, y)

    first = xl * CHIP
    half = xl * CHIP + core * HALF
    early = 2048

    def rows_of(start, size):
        return pl.ds(pl.multiple_of(start, 128), size)

    loads = [
        pltpu.make_async_copy(omega, omegas.at[0], local.at[0]),
        pltpu.make_async_copy(phase, phases.at[0], local.at[1]),
        pltpu.make_async_copy(
            samples.at[rows_of(first, early), :], sample.at[pl.ds(0, early), :], local.at[2]
        ),
        pltpu.make_async_copy(w_in, w, local.at[3]),
        pltpu.make_async_copy(
            samples.at[rows_of(first + early, CHIP - early), :],
            sample.at[pl.ds(early, CHIP - early), :],
            local.at[4],
        ),
        pltpu.make_async_copy(u_in, u, local.at[5]),
        pltpu.make_async_copy(z_in, z, local.at[6]),
        pltpu.make_async_copy(targets.at[:, rows_of(half, HALF)], tgt, local.at[7]),
        pltpu.make_async_copy(
            member.at[pl.ds(pl.multiple_of(half // 128, 16), 16), :], mem, local.at[8]
        ),
        pltpu.make_async_copy(factors, low, local.at[9]),
    ]
    for load in loads:
        load.start()

    barrier = pltpu.get_barrier_semaphore()
    for k in range(1, FEATS * ROWS):
        pl.semaphore_signal(barrier, inc=1, device_id=group_device(k), device_id_type=MESH)
    for k in range(1, REGIONS):
        pl.semaphore_signal(barrier, inc=1, device_id=region_device(k), device_id_type=MESH)
    pl.semaphore_signal(barrier, inc=1, device_id=beside, device_id_type=MESH)

    with scope("load"):
        for load in loads[:3]:
            load.wait()

    scale = math.sqrt(2.0 / FEATURES)
    c1, c3, c5 = (-scale * c for c in SINE)

    def make_rhs(side):
        turns = omegas[side].astype(F32) * (0.5 / math.pi)
        high = turns.astype(BF16)
        rest = (turns - high.astype(F32)).astype(BF16)
        for n in range(8):
            rhs[n, pl.ds(0, INPUTS), :] = high[:, n * 128 : n * 128 + 128]
            rhs[n, pl.ds(INPUTS, INPUTS), :] = rest[:, n * 128 : n * 128 + 128]

    def turns_of(row, n):
        block = sample[rows_of(row, 256), :]
        return dot(
            jnp.concatenate([block, block], axis=1),
            jnp.concatenate([rhs[2 * n], rhs[2 * n + 1]], axis=1),
        )

    def weights_of(it, side):
        return weights[it, side].reshape(OUTPUTS, BLOCK)

    def make_features(side, base, count, predicting):
        feat = feat_other if side else feat_mine
        turned = turned_other if side else turned_mine
        shift = phases[side] * (0.5 / math.pi)
        turns_next[...] = turns_of(base, 0)

        def body(i, _):
            tiles = [(m, n) for m in range(2) for n in range(4)]
            now = turns_next[...]
            total = None
            for t, (m, n) in enumerate(tiles):
                row = base + i * 512 + m * 256
                if t + 1 < len(tiles):
                    later = turns_of(base + i * 512 + tiles[t + 1][0] * 256, tiles[t + 1][1])
                else:
                    later = turns_of(base + jnp.minimum(i + 1, count - 1) * 512, 0)
                pieces = []
                for q in range(PIECES):
                    size = 256 // PIECES
                    turn = now[q * size : q * size + size] + shift[:, n * 256 : n * 256 + 256]
                    g = jnp.abs(turn - jnp.round(turn)) - 0.25
                    s = g * g
                    piece = (g * (c1 + s * (c3 + s * c5))).astype(BF16)
                    rows = pl.ds(pl.multiple_of(row + q * size, size), size)
                    feat[2 * n, rows, :] = piece[:, :128]
                    feat[2 * n + 1, rows, :] = piece[:, 128:]
                    pieces.append(piece)
                value = jnp.concatenate(pieces, axis=0).T
                cols = pl.ds(n * 256, 256)
                block = row // 128
                turned[block, cols, :] = value[:, :128]
                turned[block + 1, cols, :] = value[:, 128:]
                if predicting:
                    some = slice(n * 256, n * 256 + 256)
                    before = jnp.concatenate(
                        [turned_mine[block, cols, :], turned_mine[block + 1, cols, :]], axis=1
                    )
                    part = dot(weights_of(0, 0)[:, some], before)
                    part += dot(weights_of(0, 1)[:, some], value)
                    total = part if n == 0 else total + part
                    if n == 3:
                        pred[:, rows_of(row, 256)] = total
                now = later
            turns_next[...] = now
            return 0

        lax.fori_loop(0, count, body, 0)

    with scope("features_mine"):
        make_rhs(0)
        make_features(0, 0, early // 512, False)

    with scope("barrier"):
        pl.semaphore_wait(barrier, 31)

    om = [
        remote(
            omegas.at[0, pl.ds(0, 32), :],
            omegas.at[1, pl.ds(0, 32), :],
            om_s.at[0],
            om_r.at[0],
            across,
        ),
        remote(
            omegas.at[0, pl.ds(32, 96), :],
            omegas.at[1, pl.ds(32, 96), :],
            om_s.at[1],
            om_r.at[1],
            beside,
        ),
        remote(phases.at[0], phases.at[1], om_s.at[2], om_r.at[2], across),
    ]
    sent = []

    def start(copies, whole, send, recv):
        for copy in copies:
            copy.start()
        if send is not None:
            sent.append((whole, send, recv))

    def arrived(whole, send, recv):
        remote(whole, whole, send, recv, partner).wait_recv()

    def gather(it):
        for side, count in ((0, 3), (1, 4)):
            start(
                [
                    remote(
                        weights.at[it, 0, y],
                        weights.at[it, side, y],
                        ag_s.at[it, side],
                        ag_r.at[it, side],
                        chip_device(k),
                    )
                    for k in FAR_CHIPS[side]
                ],
                weights.at[it, side, pl.ds(0, count)],
                ag_s.at[it, side],
                ag_r.at[it, side],
            )

    def gather_wait(it, side):
        arrived(
            weights.at[it, side, pl.ds(0, 3 + side)], ag_s.at[it, side], ag_r.at[it, side]
        )

    def to_regions(source, buffer, it, send, recv):
        start(
            [
                remote(
                    source(lax.rem(reg + k, REGIONS)),
                    buffer.at[it, reg],
                    send.at[it],
                    recv.at[it],
                    region_device(k),
                )
                for k in FAR_REGIONS
            ],
            buffer.at[it, pl.ds(0, REGIONS - 1)],
            send.at[it],
            recv.at[it],
        )

    def from_regions(buffer, it, send, recv):
        arrived(buffer.at[it, pl.ds(0, REGIONS - 1)], send.at[it], recv.at[it])

    def send_rho(it, rho):
        rhos[it, reg] = jnp.broadcast_to(rho, (1, 128))
        to_regions(lambda _: rhos.at[it, reg], rhos, it, ro_s, ro_r)

    loads[3].wait()
    weights[0, 0, y] = w[...].astype(BF16)
    gather(0)
    for copy in om:
        copy.start()
    rho = jnp.full((1, 1), rho_in[0], F32)
    send_rho(0, rho)

    loads[4].wait()
    with scope("features_mine_rest"):
        make_features(0, early, (CHIP - early) // 512, False)

    with scope("omega_wait"):
        for copy in om:
            copy.wait_recv()

    eye = lax.broadcasted_iota(jnp.int32, (128, 128), 0) == lax.broadcasted_iota(
        jnp.int32, (128, 128), 1
    )

    def make_inverse():
        ys, qs, columns, lanes = [], [], [], []
        inv[...] = jnp.zeros_like(inv)
        inv_t[...] = jnp.zeros_like(inv_t)
        for b in range(8):
            at = pl.ds(b * 128, 128)
            block = low[at, at]
            diagonal = jnp.where(eye, block, 0.0)
            column = 1.0 / jnp.sum(diagonal, axis=1, keepdims=True)
            lanes.append(1.0 / jnp.sum(diagonal, axis=0, keepdims=True))
            columns.append(column)
            n = jnp.where(eye, 0.0, block) * column
            ys.append(-n)
            qs.append(dot(n.astype(BF16), n.astype(BF16)))
        for step in range(6):
            for b in range(8):
                q = qs[b].astype(BF16)
                if step < 5:
                    both = dot(jnp.concatenate([ys[b].astype(BF16), q], axis=0), q)
                    ys[b] = ys[b] + qs[b] + both[:128]
                    qs[b] = both[128:]
                else:
                    ys[b] = ys[b] + qs[b] + dot(ys[b].astype(BF16), q)
        for b in range(8):
            inv[b, pl.ds(b * 128, 128), :] = ys[b].astype(BF16)

        def square(top, size):
            return jnp.concatenate(
                [inv[top // 128 + i, pl.ds(top, size), :] for i in range(size // 128)], axis=1
            )

        size = 128
        while size < BLOCK:
            for top in range(0, BLOCK, 2 * size):
                column = jnp.concatenate(
                    columns[(top + size) // 128 : (top + 2 * size) // 128], axis=0
                )
                c = low[pl.ds(top + size, size), pl.ds(top, size)] * column
                t = c + dot(square(top + size, size), c.astype(BF16))
                t = (-t - dot(t.astype(BF16), square(top, size))).astype(BF16)
                for i in range(size // 128):
                    inv[top // 128 + i, pl.ds(top + size, size), :] = t[:, i * 128 : i * 128 + 128]
            size *= 2
        for r in range(8):
            for b in range(r + 1):
                inv_t[r, pl.ds(b * 128, 128), :] = inv[b, pl.ds(r * 128, 128), :].T
        return jnp.concatenate(lanes, axis=1)

    def predict(it, side, base, count, more):
        turned = turned_other if side else turned_mine
        for m in range(count):
            rows = rows_of(base + m * 256, 256)
            block = base // 128 + 2 * m
            part = dot(
                weights_of(it, side), jnp.concatenate([turned[block], turned[block + 1]], axis=1)
            )
            pred[:, rows] = pred[:, rows] + part if more else part

    def scale_to(value, shape):
        return jnp.broadcast_to(value, shape)

    def consensus_send(it, rho):
        value = scale_to(rho, (SLICE, BLOCK)) * (w[...] + u[...])
        for k in range(REGIONS):
            r, c = divmod(k, 8)
            cons_src[it, k] = value[r * 8 : r * 8 + 8, c * 128 : c * 128 + 128]
        cons_sum[it, reg] = cons_src[it, reg]
        to_regions(lambda r: cons_src.at[it, r], cons_sum, it, cs_s, cs_r)

    def consensus_sum(it):
        with scope("sum_wait"):
            from_regions(cons_sum, it, cs_s, cs_r)
            from_regions(rhos, it, ro_s, ro_r)
        total, divisor = cons_sum[it, 0], rhos[it, 0]
        for k in range(1, REGIONS):
            total = total + cons_sum[it, k]
            divisor = divisor + rhos[it, k]
        cons_all[it, reg] = total / divisor
        to_regions(lambda _: cons_all.at[it, reg], cons_all, it, ca_s, ca_r)

    def consensus_take(it):
        with scope("take_wait"):
            from_regions(cons_all, it, ca_s, ca_r)
        gap = jnp.zeros((8, 128), F32)
        drift = jnp.zeros((8, 128), F32)
        for k in range(REGIONS):
            r, c = divmod(k, 8)
            at = (pl.ds(r * 8, 8), pl.ds(c * 128, 128))
            new = cons_all[it, k]
            apart = w[at] - new
            moved = new - z[at]
            gap += apart * apart
            drift += moved * moved
            u[at] = u[at] + apart
            z[at] = new
        row = lax.broadcasted_iota(jnp.int32, (2, 128), 0)
        gap = scale_to(jnp.sum(gap, axis=0, keepdims=True), (2, 128))
        drift = scale_to(jnp.sum(drift, axis=0, keepdims=True), (2, 128))
        me = f * ROWS + y
        gaps[it, me] = jnp.where(row == 0, gap, drift)
        start(
            [
                remote(gaps.at[it, me], gaps.at[it, me], gp_s.at[it], gp_r.at[it], group_device(k))
                for k in FAR_GROUP
            ],
            gaps.at[it, pl.ds(0, FEATS * ROWS - 1)],
            gp_s.at[it],
            gp_r.at[it],
        )

    def penalty(it, rho):
        with scope("gap_wait"):
            arrived(gaps.at[it, pl.ds(0, FEATS * ROWS - 1)], gp_s.at[it], gp_r.at[it])
        total = gaps[it, 0]
        for k in range(1, FEATS * ROWS):
            total = total + gaps[it, k]
        total = jnp.sum(total, axis=1, keepdims=True)
        offset = 0.01 * FEATURES * OUTPUTS
        gap, drift = total[0:1], rho * rho * total[1:2]
        new = rho * jnp.sqrt((gap + offset) / (drift + offset))
        u[...] = u[...] * scale_to(rho / new, (SLICE, BLOCK))
        pen_out[:, it : it + 1] = new
        return new

    mine_at = core * HALF
    other_at = (1 - core) * HALF
    lanes = None
    for it in range(ITERS):
        if it == 0:
            with scope("gather_wait"):
                gather_wait(0, 0)
                gather_wait(0, 1)
            with scope("features_other"):
                make_rhs(1)
                make_features(1, other_at, 4, True)
        else:
            with scope("gather_wait"):
                gather_wait(it, 0)
            with scope("predict_first"):
                predict(it, 0, 0, 16, False)
            if it > 1:
                consensus_sum(it - 1)
            with scope("gather_wait"):
                gather_wait(it, 1)
            with scope("predict_other"):
                predict(it, 1, other_at, 8, True)
        for g in range(HALF // 128):
            pred_send[it, g] = pred[:, rows_of(other_at + g * 128, 128)].astype(BF16)
        to_pair = remote(
            pred_send.at[it], pred_recv.at[it], pair_s.at[it, 0], pair_r.at[it, 0], partner
        )
        start([to_pair], pred_send.at[it], pair_s.at[it, 0], pair_r.at[it, 0])
        if it == 0:
            with scope("features_other_rest"):
                make_features(1, mine_at, 4, True)
            for load in loads[5:]:
                load.wait()
        else:
            if it == 1:
                consensus_sum(it - 1)
            with scope("predict_mine"):
                predict(it, 1, mine_at, 8, True)
        with scope("pred_wait"):
            to_pair.wait_recv()
        with scope("residual"):
            for g in range(HALF // 128):
                value = pred[:, rows_of(mine_at + g * 128, 128)] + pred_recv[it, g].astype(F32)
                value = value - tgt[:, g * 128 : g * 128 + 128].astype(F32)
                res_own[it, g] = (mem[g : g + 1, :].astype(F32) * value).astype(BF16)
        res = remote(res_own.at[it], res_other.at[it], pair_s.at[it, 1], pair_r.at[it, 1], partner)
        start([res], res_own.at[it], pair_s.at[it, 1], pair_r.at[it, 1])

        def gradient_part(residual, feat, at, n):
            rows = rows_of(at, HALF)
            return dot(
                jnp.concatenate([residual[it, g] for g in range(HALF // 128)], axis=1),
                jnp.concatenate([feat[2 * n, rows, :], feat[2 * n + 1, rows, :]], axis=1),
            )

        with scope("gradient_mine"):
            for side, feat in ((1, feat_other), (0, feat_mine)):
                for n in range(4):
                    acc[side, :, pl.ds(n * 256, 256)] = gradient_part(res_own, feat, mine_at, n)
        with scope("res_wait"):
            res.wait_recv()
        for side, feat in ((1, feat_other), (0, feat_mine)):
            for part in range(2):
                with scope("gradient_other"):
                    for n in range(2 * part, 2 * part + 2):
                        cols = pl.ds(n * 256, 256)
                        total = acc[side, :, cols] + gradient_part(res_other, feat, other_at, n)
                        grad_send[it, side, :, :, cols] = total.reshape(ROWS, SLICE, 256).astype(BF16)
                cols = pl.ds(part * 512, 512)
                start(
                    [
                        remote(
                            grad_send.at[it, side, chip(k)[1], :, cols],
                            grad_recv.at[it, k, :, cols],
                            rs_s.at[it],
                            rs_r.at[it],
                            chip_device(k),
                        )
                        for k in FAR_CHIPS[side]
                    ],
                    grad_recv.at[it, pl.ds(1, 7)],
                    rs_s.at[it] if side == 0 and part == 1 else None,
                    rs_r.at[it],
                )
        if it == 0:
            with scope("inverse"):
                lanes = make_inverse()
        else:
            consensus_take(it - 1)
        old_rho_u = scale_to(rho, (SLICE, BLOCK)) * u[...]
        gradient = grad_send[it, 0, y].astype(F32)
        with scope("grad_wait"):
            arrived(grad_recv.at[it, pl.ds(1, 7)], rs_s.at[it], rs_r.at[it])
        with scope("solve"):
            for k in range(1, 8):
                gradient = gradient + grad_recv[it, k].astype(F32)
            right = jnp.concatenate([gradient + old_rho_u, w[...] - z[...]], axis=0) * lanes
            low16 = right.astype(BF16)
            right = right + jnp.concatenate(
                [
                    dot(
                        low16[:, : n * 256 + 256],
                        jnp.concatenate(
                            [inv_t[2 * n + i, pl.ds(0, n * 256 + 256), :] for i in range(2)], axis=1
                        ),
                    )
                    for n in range(4)
                ],
                axis=1,
            )
            low16 = right.astype(BF16)
            right = right + jnp.concatenate(
                [
                    dot(
                        low16[:, n * 256 :],
                        jnp.concatenate(
                            [
                                inv[2 * n + i, pl.ds(n * 256, BLOCK - n * 256), :]
                                for i in range(2)
                            ],
                            axis=1,
                        ),
                    )
                    for n in range(4)
                ],
                axis=1,
            )
            right = right * lanes
        if it:
            rho = penalty(it - 1, rho)
        new = w[...] - right[:SLICE] - scale_to(rho, (SLICE, BLOCK)) * right[SLICE:]
        w[...] = new
        with scope("consensus_send"):
            consensus_send(it, rho)
        if it < ITERS - 1:
            weights[it + 1, 0, y] = new.astype(BF16)
            gather(it + 1)
        if it:
            send_rho(it, rho)

    consensus_sum(ITERS - 1)
    consensus_take(ITERS - 1)
    penalty(ITERS - 1, rho)
    for copy in om:
        copy.wait_send()
    for whole, send, recv in sent:
        remote(whole, whole, send, recv, partner).wait_send()


def hand_over(*refs):
    for source, out in zip(refs[:4], refs[4:]):
        out[...] = source[...]


def per_device(
    samples,
    targets,
    member,
    omega,
    phase,
    factors,
    weights_init,
    duals_init,
    consensus_init,
    penalty_init,
):
    hbm = pl.BlockSpec(memory_space=pl.ANY)
    vmem = pl.BlockSpec(memory_space=pltpu.VMEM)
    smem = pl.BlockSpec(memory_space=pltpu.SMEM)
    state = jax.ShapeDtypeStruct((SLICE, BLOCK), F32)
    dma = pltpu.SemaphoreType.DMA
    w, u, z, pen = pl.pallas_call(
        kernel,
        out_shape=(state, state, state, jax.ShapeDtypeStruct((1, ITERS), F32)),
        in_specs=[hbm] * 9 + [smem],
        out_specs=(vmem,) * 4,
        scratch_shapes=[
            pltpu.VMEM((8, CHIP, 128), BF16),
            pltpu.VMEM((8, CHIP, 128), BF16),
            pltpu.VMEM((CHIP // 128, BLOCK, 128), BF16),
            pltpu.VMEM((CHIP // 128, BLOCK, 128), BF16),
            pltpu.VMEM((CHIP, INPUTS), BF16),
            pltpu.VMEM((2, INPUTS, BLOCK), BF16),
            pltpu.VMEM((2, 1, BLOCK), F32),
            pltpu.VMEM((8, 2 * INPUTS, 128), BF16),
            pltpu.VMEM((256, 256), F32),
            pltpu.VMEM((OUTPUTS, HALF), BF16),
            pltpu.VMEM((16, 128), jnp.int32),
            pltpu.VMEM((BLOCK, BLOCK), F32),
            pltpu.VMEM((8, BLOCK, 128), BF16),
            pltpu.VMEM((8, BLOCK, 128), BF16),
            pltpu.VMEM((ITERS, 2, ROWS, SLICE, BLOCK), BF16),
            pltpu.VMEM((OUTPUTS, CHIP), F32),
            pltpu.VMEM((ITERS, 16, OUTPUTS, 128), BF16),
            pltpu.VMEM((ITERS, 16, OUTPUTS, 128), BF16),
            pltpu.VMEM((ITERS, 16, OUTPUTS, 128), BF16),
            pltpu.VMEM((ITERS, 16, OUTPUTS, 128), BF16),
            pltpu.VMEM((2, OUTPUTS, BLOCK), F32),
            pltpu.VMEM((ITERS, 2, ROWS, SLICE, BLOCK), BF16),
            pltpu.VMEM((ITERS, 8, SLICE, BLOCK), BF16),
            pltpu.VMEM((ITERS, REGIONS, 8, 128), F32),
            pltpu.VMEM((ITERS, REGIONS, 8, 128), F32),
            pltpu.VMEM((ITERS, REGIONS, 8, 128), F32),
            pltpu.VMEM((ITERS, REGIONS, 1, 128), F32),
            pltpu.VMEM((ITERS, FEATS * ROWS, 2, 128), F32),
            dma((10,)),
            dma((3,)),
            dma((3,)),
            dma((ITERS, 2)),
            dma((ITERS, 2)),
            dma((ITERS,)),
            dma((ITERS,)),
            dma((ITERS, 2)),
            dma((ITERS, 2)),
            dma((ITERS,)),
            dma((ITERS,)),
            dma((ITERS,)),
            dma((ITERS,)),
            dma((ITERS,)),
            dma((ITERS,)),
            dma((ITERS,)),
            dma((ITERS,)),
        ],
        compiler_params=pltpu.CompilerParams(
            collective_id=0, has_side_effects=True, vmem_limit_bytes=60 * 1024 * 1024
        ),
        name="admm",
    )(
        samples,
        targets.T,
        member.reshape(64, 128),
        omega,
        phase.reshape(1, BLOCK),
        factors,
        weights_init.T,
        duals_init.T,
        consensus_init.T,
        penalty_init,
    )
    w, u, z, pen = pl.pallas_call(
        hand_over,
        out_shape=(state, state, state, jax.ShapeDtypeStruct((1, ITERS), F32)),
        in_specs=[vmem] * 4,
        out_specs=(vmem,) * 4,
        name="hand_over",
    )(w, u, z, pen)
    return w.T, u.T, z.T, pen


def solution(mesh):
    return jax.shard_map(
        per_device,
        mesh=mesh,
        in_specs=(
            P(("region", "row"), None),
            P(("region", "row"), None),
            P(("region", "row")),
            P(None, "feat"),
            P("feat"),
            P(("region", "feat"), None),
            P(("region", "feat"), "row"),
            P(("region", "feat"), "row"),
            P("feat", "row"),
            P("region"),
        ),
        out_specs=(
            P(("region", "feat"), "row"),
            P(("region", "feat"), "row"),
            P("feat", "row"),
            P("region", None),
        ),
        check_vma=False,
    )
```
